16 devices in a mesh: dp: 4 (over y, z, core), sp: 4 (over x).
Axes of the slice: x: 4, y: 2, z: 1, core: 2. Of those that a mesh axis runs over, the one named last changes fastest.
The devices are a block of a 4x4x8 slice.
Arguments:
- x: bfloat16 [4096, 2048], P(('dp', 'sp')), parts along dimension 0
- gain: bfloat16 [2048], replicated
- wq: bfloat16 [2048, 4096], replicated
- wk: bfloat16 [2048, 512], replicated
- wv: bfloat16 [2048, 512], replicated
- wo: bfloat16 [4096, 2048], replicated
Outputs:
- output: bfloat16 [4096, 2048], P(('dp', 'sp')), parts along dimension 0
There are 4 independent parts. The reference program is written for one: setup_inputs(seed, part) draws one part's arguments, and reference() takes and returns one part's arrays. A program takes and returns all parts, laid end to end along the dimension named above; an argument that names none is the same for every part.
All inputs are finite; a program needn't handle non-finite values.
Results may differ from the reference program's by a relative error of at most 0.012.
Values are sent between devices in bfloat16 or wider.
A program may use at most 768 MiB of HBM per device.

```python
import jax
import jax.numpy as jnp
from jax import lax

ROWS = 1024
D = 2048
HEADS = 16
KV_HEADS = 2
HEAD = 256
THETA = 10000


def setup_inputs(seed: int = 0, part: int = 0) -> dict:
    kx, kn, kq, kk, kv, ko = jax.random.split(jax.random.key(seed), 6)

    def weights(key, rows, columns):
        return jax.random.normal(key, (rows, columns), jnp.float32) * rows**-0.5

    drawn = {
        "x": jax.random.normal(jax.random.fold_in(kx, part), (ROWS, D), jnp.float32),
        "gain": 1 + 0.1 * jax.random.normal(kn, (D,), jnp.float32),
        "wq": 2 * weights(kq, D, HEADS * HEAD),
        "wk": 2 * weights(kk, D, KV_HEADS * HEAD),
        "wv": 4 * weights(kv, D, KV_HEADS * HEAD),
        "wo": weights(ko, HEADS * HEAD, D),
    }
    return {k: v.astype(jnp.bfloat16) for k, v in drawn.items()}


def normed(x, gain):
    wide = x.astype(jnp.float32)
    scale = lax.rsqrt(jnp.mean(wide * wide, -1, keepdims=True) + 1e-6)
    return (wide * scale * gain.astype(jnp.float32)).astype(jnp.bfloat16)


def turned(t, place, theta):
    half = t.shape[-1] // 2
    angle = place.astype(jnp.float32)[:, None] * theta ** (-jnp.arange(half, dtype=jnp.float32) / half)
    cos, sin = jnp.cos(angle)[:, None], jnp.sin(angle)[:, None]
    a, b = t[..., :half].astype(jnp.float32), t[..., half:].astype(jnp.float32)
    return jnp.concatenate([a * cos - b * sin, b * cos + a * sin], -1).astype(jnp.bfloat16)


def matmul(a, w):
    return jnp.dot(a, w, preferred_element_type=jnp.float32).astype(jnp.bfloat16)


def einsum(form, a, b):
    return jnp.einsum(form, a.astype(jnp.float32), b.astype(jnp.float32))


def attention(q, k, v):
    scores = einsum("tgsd,ugd->gstu", q, k) * q.shape[-1] ** -0.5
    token = jnp.arange(q.shape[0])
    scores = jnp.where(token[:, None] >= token, scores, -jnp.inf)
    weights = jax.nn.softmax(scores, -1).astype(jnp.bfloat16)
    return einsum("gstu,ugd->tgsd", weights, v).astype(jnp.bfloat16)


def reference(x, gain, wq, wk, wv, wo):
    a, place = normed(x, gain), jnp.arange(ROWS)
    q = turned(matmul(a, wq).reshape(ROWS, HEADS, HEAD), place, THETA).reshape(ROWS, KV_HEADS, -1, HEAD)
    k = turned(matmul(a, wk).reshape(ROWS, KV_HEADS, HEAD), place, THETA)
    v = matmul(a, wv).reshape(ROWS, KV_HEADS, HEAD)
    seen = attention(q, k, v).reshape(ROWS, HEADS * HEAD)
    return (x.astype(jnp.float32) + jnp.dot(seen, wo, preferred_element_type=jnp.float32)).astype(jnp.bfloat16)
```

```python
import functools

import jax
import jax.numpy as jnp
import numpy as np
from jax import lax
from jax.experimental import pallas as pl
from jax.experimental.pallas import tpu as pltpu
from jax.sharding import PartitionSpec as P

HEAD = 256
THETA = 10000
LOG2E = 1.4426950408889634
NEG = -1e30
VMEM_LIMIT = 67_000_000
MESH = pl.DeviceIdType.MESH


def _dot(a, b, ca=1, cb=0):
    return lax.dot_general(a, b, (((ca,), (cb,)), ((), ())), preferred_element_type=jnp.float32)


def _kernel(x_hbm, gain_hbm, cos_hbm, sin_hbm, wq_hbm, wk_hbm, wv_hbm, wo_hbm, y_hbm,
            x_s, gain_s, cos_s, sin_s, wk_s, wv_s, wq_s, wo_s, a_s, q_s, kv_s, acc_s, m_s, l_s, o_s, y_s, out_s,
            in_sem, wk_sem, wv_sem, wq_sem, wo_sem, send_sem, recv_sem, out_sem, *, n):
    own, d = x_s.shape
    kv_heads, per = q_s.shape[0], q_s.shape[1] // own
    half_rows = own // 2
    hh = HEAD // 2
    tile = out_s.shape[2]
    tiles = d // tile
    me = lax.axis_index("sp")
    right, left = lax.rem(me + 1, n), lax.rem(me + n - 1, n)

    def x_in():
        return pltpu.make_async_copy(x_hbm, x_s, in_sem.at[0])

    def gain_in():
        return pltpu.make_async_copy(gain_hbm, gain_s, in_sem.at[1])

    def cos_in():
        return pltpu.make_async_copy(cos_hbm.at[pl.ds(me * own, own)], cos_s, in_sem.at[2])

    def sin_in():
        return pltpu.make_async_copy(sin_hbm.at[pl.ds(me * own, own)], sin_s, in_sem.at[3])

    def cols(i, width):
        return pl.ds(pl.multiple_of(i * width, width), width)

    def wk_in(h):
        return pltpu.make_async_copy(wk_hbm.at[:, cols(h, HEAD)], wk_s.at[h], wk_sem.at[h])

    def wv_in(h):
        return pltpu.make_async_copy(wv_hbm.at[:, cols(h, HEAD)], wv_s.at[h], wv_sem.at[h])

    def wq_in(i):
        return pltpu.make_async_copy(wq_hbm.at[:, cols(i, HEAD)], wq_s.at[i], wq_sem.at[i])

    def wo_in(h, t):
        return pltpu.make_async_copy(wo_hbm.at[cols(h, per * HEAD), cols(t, tile)], wo_s.at[h, t], wo_sem.at[h, t])

    x_in().start()
    gain_in().start()
    for h in range(kv_heads):
        wk_in(h).start()
        wv_in(h).start()
    cos_in().start()
    sin_in().start()
    ahead = 6
    for i in range(ahead):
        wq_in(i).start()

    barrier = pltpu.get_barrier_semaphore()
    for peer in (left, right):
        pl.semaphore_signal(barrier, inc=1, device_id={"sp": peer}, device_id_type=MESH)

    x_in().wait()
    gain_in().wait()
    wide = x_s[...].astype(jnp.float32)
    scale = lax.rsqrt(jnp.mean(wide * wide, -1, keepdims=True) + 1e-6)
    a_s[...] = (wide * scale * gain_s[...].astype(jnp.float32).reshape(1, d)).astype(jnp.bfloat16)
    cos_in().wait()
    sin_in().wait()

    def turn(t):
        t = t.astype(jnp.bfloat16).astype(jnp.float32)
        a, b = t[:, :hh], t[:, hh:]
        cos, sin = cos_s[...], sin_s[...]
        return (a * cos - b * sin).astype(jnp.bfloat16), (b * cos + a * sin).astype(jnp.bfloat16)

    def piece(block, h, c):
        return kv_s.at[block, h, pl.ds(c * half_rows, half_rows)]

    def push(block, h, c, to, way):
        return pltpu.make_async_remote_copy(
            src_ref=piece(block, h, c), dst_ref=piece(block, h, c), send_sem=send_sem.at[way, block, h, c],
            recv_sem=recv_sem.at[block, h, c], device_id={"sp": to}, device_id_type=MESH)

    def arrived(block, h, c):
        push(block, h, c, right, 0).wait_recv()

    pl.semaphore_wait(barrier, 2)

    for h in range(kv_heads):
        wk_in(h).wait()
        k1, k2 = turn(_dot(a_s[...], wk_s[h]))
        kv_s[me, h, :, :hh] = k1
        kv_s[me, h, :, hh:HEAD] = k2
        wv_in(h).wait()
        kv_s[me, h, :, HEAD:] = _dot(a_s[...], wv_s[h]).astype(jnp.bfloat16)

        @pl.when(me == 0)
        def _():
            for c in range(2):
                push(0, h, c, left, 1).start()
                push(0, h, c, right, 0).start()

        @pl.when(me == 1)
        def _():
            push(1, h, 1, left, 1).start()
            push(1, h, 0, right, 0).start()
            push(1, h, 1, right, 0).start()

        @pl.when(me == 2)
        def _():
            for c in range(2):
                push(2, h, c, right, 0).start()

    def query(i, _):
        @pl.when(i + ahead < kv_heads * per)
        def _():
            wq_in(i + ahead).start()

        @pl.when(i + ahead >= kv_heads * per)
        def _():
            wo_in(lax.div(i + ahead - kv_heads * per, tiles), lax.rem(i + ahead - kv_heads * per, tiles)).start()

        wq_in(i).wait()
        q1, q2 = turn(_dot(a_s[...], wq_s[i]))
        rows = pl.ds(pl.multiple_of(lax.rem(i, per) * own, own), own)
        q_s[lax.div(i, per), rows, :hh] = q1
        q_s[lax.div(i, per), rows, hh:] = q2

    lax.fori_loop(0, kv_heads * per, query, None)
    for j in range(ahead, kv_heads * tiles):
        wo_in(j // tiles, j % tiles).start()

    @pl.when(me == 0)
    def _():
        for h in range(kv_heads):
            arrived(1, h, 1)
            push(1, h, 1, left, 1).start()

    @pl.when(me == n - 1)
    def _():
        for c in range(2):
            arrived(0, 0, c)
            push(0, 0, c, left, 1).start()

    e = HEAD**-0.5 * LOG2E
    strip = 2 * own

    def attend(block, h, diagonal):
        k = kv_s[block, h, :, :HEAD]
        v = kv_s[block, h, :, HEAD:]
        if diagonal:
            row = lax.rem(lax.broadcasted_iota(jnp.int32, (strip, own), 0), own)
            seen = row >= lax.broadcasted_iota(jnp.int32, (strip, own), 1)
        for at in range(0, per * own, strip):
            here = slice(at, at + strip)
            s = _dot(q_s[h, here], k, 1, 1)
            if diagonal:
                s = jnp.where(seen, s, NEG)
                top = jnp.max(s, axis=1, keepdims=True)
            else:
                old = m_s[h, here][:, :1]
                top = jnp.maximum(old, jnp.max(s, axis=1, keepdims=True))
            p = jnp.exp2((s - top) * e)
            part = p[:, :128]
            for j in range(128, own, 128):
                part = part + p[:, j:j + 128]
            mix = _dot(p.astype(jnp.bfloat16), v)
            m_s[h, here] = jnp.broadcast_to(top, (strip, 128))
            if diagonal:
                l_s[h, here] = part
                acc_s[h, here] = mix
            else:
                keep = jnp.exp2((old - top) * e)
                l_s[h, here] = l_s[h, here] * keep + part
                acc_s[h, here] = acc_s[h, here] * keep + mix

    def project(h):
        for r in range(per):
            here = slice(r * own, (r + 1) * own)
            total = jnp.sum(l_s[h, here], axis=1, keepdims=True)
            o_s[:, r * HEAD:(r + 1) * HEAD] = (acc_s[h, here] * (1 / total)).astype(jnp.bfloat16)
        for t in range(tiles):
            wo_in(h, t).wait()

        def columns(t, _):
            y = _dot(o_s[...], wo_s[h, t])

            @pl.when(h == 0)
            def _():
                y_s[t] = y

            @pl.when(h == kv_heads - 1)
            def _():
                here = cols(t, tile)
                out_s[t] = (x_s[:, here].astype(jnp.float32) + (y_s[t] + y)).astype(jnp.bfloat16)
                pltpu.make_async_copy(out_s.at[t], y_hbm.at[:, here], out_sem.at[t]).start()

        lax.fori_loop(0, tiles, columns, None)

    def own_block(h, _):
        attend(me, h, True)

        @pl.when(me == 0)
        def _():
            project(h)

    lax.fori_loop(0, kv_heads, own_block, None)

    def other(u, _):
        s, h = lax.div(u, kv_heads), lax.rem(u, kv_heads)

        @pl.when(me > s)
        def _():
            block = jnp.where(s == 0, me - 1, s - 1)
            for c in range(2):
                @pl.when(jnp.logical_not((me == n - 1) & (block == 0) & (h == 0)))
                def _():
                    arrived(block, h, c)

                @pl.when((me == 2) & (block == 1) & (c == 0))
                def _():
                    push(1, h, 0, right, 0).start()

                @pl.when((me == n - 1) & (block == 0) & (h > 0))
                def _():
                    push(0, h, c, left, 1).start()

            attend(block, h, False)

            @pl.when(s == me - 1)
            def _():
                project(h)

    lax.fori_loop(0, (n - 1) * kv_heads, other, None)

    for t in range(tiles):
        pltpu.make_async_copy(out_s.at[t], y_hbm.at[:, t * tile:(t + 1) * tile], out_sem.at[t]).wait()
    for h in range(kv_heads):
        for c in range(2):
            @pl.when(me == 0)
            def _():
                push(0, h, c, left, 1).wait_send()
                push(0, h, c, right, 0).wait_send()

            @pl.when(me == 1)
            def _():
                push(1, h, c, right, 0).wait_send()

            @pl.when(me == 2)
            def _():
                push(2, h, c, right, 0).wait_send()

            @pl.when(me == n - 1)
            def _():
                push(0, h, c, left, 1).wait_send()

        @pl.when((me == 0) | (me == 1))
        def _():
            push(1, h, 1, left, 1).wait_send()

        @pl.when(me == 2)
        def _():
            push(1, h, 0, right, 0).wait_send()


def solution(mesh):
    n = mesh.shape["sp"]

    def step(x, gain, wq, wk, wv, wo):
        own, d = x.shape
        heads, kv_heads = wq.shape[1] // HEAD, wk.shape[1] // HEAD
        per = heads // kv_heads
        tile = 512
        place = np.arange(n * own, dtype=np.float64)[:, None]
        angle = place * THETA ** (-np.arange(HEAD // 2, dtype=np.float64) / (HEAD // 2))
        cos, sin = jnp.asarray(np.cos(angle), jnp.float32), jnp.asarray(np.sin(angle), jnp.float32)
        anywhere = pl.BlockSpec(memory_space=pl.ANY)
        dma = pltpu.SemaphoreType.DMA
        bf16, f32 = jnp.bfloat16, jnp.float32
        return pl.pallas_call(
            functools.partial(_kernel, n=n),
            out_shape=jax.ShapeDtypeStruct((own, d), bf16),
            in_specs=[anywhere] * 8,
            out_specs=anywhere,
            scratch_shapes=[
                pltpu.VMEM((own, d), bf16),
                pltpu.VMEM((d,), bf16),
                pltpu.VMEM((own, HEAD // 2), f32),
                pltpu.VMEM((own, HEAD // 2), f32),
                pltpu.VMEM((kv_heads, d, HEAD), bf16),
                pltpu.VMEM((kv_heads, d, HEAD), bf16),
                pltpu.VMEM((heads, d, HEAD), bf16),
                pltpu.VMEM((kv_heads, d // tile, per * HEAD, tile), bf16),
                pltpu.VMEM((own, d), bf16),
                pltpu.VMEM((kv_heads, per * own, HEAD), bf16),
                pltpu.VMEM((n, kv_heads, own, 2 * HEAD), bf16),
                pltpu.VMEM((kv_heads, per * own, HEAD), f32),
                pltpu.VMEM((kv_heads, per * own, 128), f32),
                pltpu.VMEM((kv_heads, per * own, 128), f32),
                pltpu.VMEM((own, per * HEAD), bf16),
                pltpu.VMEM((d // tile, own, tile), f32),
                pltpu.VMEM((d // tile, own, tile), bf16),
                dma((4,)), dma((kv_heads,)), dma((kv_heads,)), dma((heads,)), dma((kv_heads, d // tile)),
                dma((2, n, kv_heads, 2)), dma((n, kv_heads, 2)), dma((d // tile,)),
            ],
            compiler_params=pltpu.CompilerParams(collective_id=0, has_side_effects=True, vmem_limit_bytes=VMEM_LIMIT),
        )(x, gain, cos, sin, wq, wk, wv, wo)

    tokens, whole = P(("dp", "sp"), None), P(None, None)
    return jax.shard_map(
        step,
        mesh=mesh,
        in_specs=(tokens, P(None), whole, whole, whole, whole),
        out_specs=tokens,
        check_vma=False,
    )
```

```python
import functools

import jax
import jax.numpy as jnp
import numpy as np
from jax import lax
from jax.experimental import pallas as pl
from jax.experimental.pallas import tpu as pltpu
from jax.sharding import PartitionSpec as P

HEAD = 256
THETA = 10000
LOG2E = 1.4426950408889634
NEG = -1e30
VMEM_LIMIT = 60 * 2**20
MESH = pl.DeviceIdType.MESH


def _dot(a, b, ca=1, cb=0):
    return lax.dot_general(a, b, (((ca,), (cb,)), ((), ())), preferred_element_type=jnp.float32)


def _kernel(x_hbm, gain_hbm, cos_hbm, sin_hbm, wq_hbm, wk_hbm, wv_hbm, wo_hbm, out_ref,
            x_s, gain_s, cos_s, sin_s, wk_s, wv_s, wq_s, wo_s, a_s, q_s, kv_s, acc_s, m_s, l_s, o_s, y_s,
            in_sem, wk_sem, wv_sem, wq_sem, wo_sem, send_sem, recv_sem, *, n):
    own, d = x_s.shape
    kv_heads, per = q_s.shape[0], q_s.shape[1] // own
    heads = kv_heads * per
    hh = HEAD // 2
    tile = wo_s.shape[3]
    tiles = d // tile
    me = lax.axis_index("sp")
    right, left = lax.rem(me + 1, n), lax.rem(me + n - 1, n)
    K, V = 0, 1

    def cols(i, width):
        return pl.ds(i * width if isinstance(i, int) else pl.multiple_of(i * width, width), width)

    x_in = pltpu.make_async_copy(x_hbm, x_s, in_sem.at[0])
    gain_in = pltpu.make_async_copy(gain_hbm, gain_s, in_sem.at[1])
    cos_in = pltpu.make_async_copy(cos_hbm.at[pl.ds(me * own, own)], cos_s, in_sem.at[2])
    sin_in = pltpu.make_async_copy(sin_hbm.at[pl.ds(me * own, own)], sin_s, in_sem.at[3])

    def wk_in(h):
        return pltpu.make_async_copy(wk_hbm.at[:, cols(h, HEAD)], wk_s.at[h], wk_sem.at[h])

    def wv_in(h):
        return pltpu.make_async_copy(wv_hbm.at[:, cols(h, HEAD)], wv_s.at[h], wv_sem.at[h])

    def wq_in(i):
        return pltpu.make_async_copy(wq_hbm.at[:, cols(i, HEAD)], wq_s.at[i], wq_sem.at[i])

    def wo_in(h, t):
        return pltpu.make_async_copy(wo_hbm.at[cols(h, per * HEAD), cols(t, tile)], wo_s.at[h, t], wo_sem.at[h, t])

    x_in.start()
    gain_in.start()
    for h in range(kv_heads):
        wk_in(h).start()
        if h == 0:
            cos_in.start()
            sin_in.start()
        wv_in(h).start()

    barrier = pltpu.get_barrier_semaphore()
    for peer in (left, right):
        pl.semaphore_signal(barrier, inc=1, device_id={"sp": peer}, device_id_type=MESH)

    x_in.wait()
    gain_in.wait()
    wide = x_s[...].astype(jnp.float32)
    scale = lax.rsqrt(jnp.mean(wide * wide, -1, keepdims=True) + 1e-6)
    a_s[...] = (wide * scale * gain_s[...].astype(jnp.float32).reshape(1, d)).astype(jnp.bfloat16)

    def turn(t):
        t = t.astype(jnp.bfloat16).astype(jnp.float32)
        a, b = t[:, :hh], t[:, hh:]
        cos, sin = cos_s[...], sin_s[...]
        return (a * cos - b * sin).astype(jnp.bfloat16), (b * cos + a * sin).astype(jnp.bfloat16)

    def push(block, h, c, way):
        return pltpu.make_async_remote_copy(
            src_ref=kv_s.at[block, h, c], dst_ref=kv_s.at[block, h, c], send_sem=send_sem.at[way, block, h, c],
            recv_sem=recv_sem.at[block, h, c], device_id={"sp": left if way else right}, device_id_type=MESH)

    R, L = 0, 1

    def arrived(block, h, c):
        push(block, h, c, R).wait_recv()

    def start_own(h, c):
        @pl.when(me == 0)
        def _():
            push(0, h, c, R).start()
            if h == 0:
                push(0, h, c, L).start()

        @pl.when(me == 1)
        def _():
            push(1, h, c, R).start()
            if c == V:
                push(1, h, c, L).start()

        if h == 0:
            @pl.when(me == 2)
            def _():
                push(2, h, c, R).start()

    def start_later():
        @pl.when(me == 0)
        def _():
            arrived(1, 0, V)
            push(1, 0, V, L).start()
            push(0, 1, K, L).start()
            push(0, 1, V, L).start()

        @pl.when(me == 2)
        def _():
            arrived(1, 0, K)
            push(1, 0, K, R).start()
            push(2, 1, K, R).start()
            push(2, 1, V, R).start()

        @pl.when(me == 3)
        def _():
            arrived(0, 0, K)
            push(0, 0, K, L).start()

    def wait_sent():
        @pl.when(me == 0)
        def _():
            for h in range(kv_heads):
                for c in (K, V):
                    push(0, h, c, R).wait_send()
                    push(0, h, c, L).wait_send()
                push(1, h, V, L).wait_send()

        @pl.when(me == 1)
        def _():
            for h in range(kv_heads):
                for c in (K, V):
                    push(1, h, c, R).wait_send()
                push(1, h, V, L).wait_send()
            for c in (K, V):
                push(0, 1, c, R).wait_send()

        @pl.when(me == 2)
        def _():
            for h in range(kv_heads):
                for c in (K, V):
                    push(2, h, c, R).wait_send()
                push(1, h, K, R).wait_send()

        @pl.when(me == 3)
        def _():
            for c in (K, V):
                push(0, 0, c, L).wait_send()

    for h in range(kv_heads):
        wk_in(h).wait()
        if h == 0:
            cos_in.wait()
            sin_in.wait()
        k1, k2 = turn(_dot(a_s[...], wk_s[h]))
        kv_s[me, h, K, :, :hh] = k1
        kv_s[me, h, K, :, hh:] = k2
        if h == 0:
            pl.semaphore_wait(barrier, 2)
        start_own(h, K)
        wv_in(h).wait()
        if h == 0:
            for i in range(heads // 2):
                wq_in(i).start()
        else:
            for i in range(heads // 2, heads):
                wq_in(i).start()
        kv_s[me, h, V] = _dot(a_s[...], wv_s[h]).astype(jnp.bfloat16)
        start_own(h, V)

    group = 4
    rounds = heads // group

    def query(i, _):
        for r in range(group):
            wq_in(i * group + r).wait()
        for r in range(wo_chunks):
            j = i * wo_chunks + r
            wo_in(lax.div(j, tiles), lax.rem(j, tiles)).start()
        for r in range(group):
            j = i * group + r
            q1, q2 = turn(_dot(a_s[...], wq_s[j]))
            rows = pl.ds(pl.multiple_of(lax.rem(j, per) * own, own), own)
            q_s[lax.div(j, per), rows, :hh] = q1
            q_s[lax.div(j, per), rows, hh:] = q2

        @pl.when(i == rounds - 2)
        def _():
            start_later()

    wo_chunks = kv_heads * tiles // rounds
    lax.fori_loop(0, rounds, query, None)
    y_s[...] = x_s[...].astype(jnp.float32)

    e = HEAD**-0.5 * LOG2E
    strips = [slice(r * own, (r + 1) * own) for r in range(per)]

    def scores(h, at, blocks, diagonal):
        out = [_dot(q_s[h, at], kv_s[b, h, K], 1, 1) for b in blocks]
        if diagonal:
            seen = lax.broadcasted_iota(jnp.int32, (own, own), 0) >= lax.broadcasted_iota(jnp.int32, (own, own), 1)
            out[0] = jnp.where(seen, out[0], NEG)
        return out

    def largest(parts, old=None):
        top = None
        for s in parts:
            for j in range(0, own, 128):
                top = s[:, j:j + 128] if top is None else jnp.maximum(top, s[:, j:j + 128])
        top = jnp.broadcast_to(jnp.max(top, axis=1, keepdims=True), (own, 128))
        return top if old is None else jnp.maximum(old, top)

    def weigh(parts, top):
        out, total = [], None
        for s in parts:
            for j in range(0, own, 128):
                p = jnp.exp2((s[:, j:j + 128] - top) * e)
                total = p if total is None else total + p
                out.append(p.astype(jnp.bfloat16))
        return jnp.concatenate(out, axis=1), total

    def twice(t):
        return jnp.concatenate([t, t], axis=1)

    def values(h, blocks):
        return jnp.concatenate([kv_s[b, h, V] for b in blocks], axis=0)

    def begin(h, blocks):
        def finish(p, at):
            acc_s[at] = _dot(p, values(h, blocks))

        later, prev = scores(h, strips[0], blocks, True), None
        for r, at in enumerate(strips):
            parts = later
            if r + 1 < per:
                later = scores(h, strips[r + 1], blocks, True)
            if prev is not None:
                finish(*prev)
            top = largest(parts)
            p, total = weigh(parts, top)
            m_s[at] = top
            l_s[at] = total
            prev = p, at
        finish(*prev)

    def end(h, block):
        def finish(p, keep, total, r, at):
            share = 1 / jnp.broadcast_to(jnp.sum(total, axis=1, keepdims=True), (own, 128))
            mix = acc_s[at] * twice(keep) + _dot(p, kv_s[block, h, V])
            o_s[:, r * HEAD:(r + 1) * HEAD] = (mix * twice(share)).astype(jnp.bfloat16)

        later, prev = scores(h, strips[0], [block], False), None
        for r, at in enumerate(strips):
            parts = later
            if r + 1 < per:
                later = scores(h, strips[r + 1], [block], False)
            if prev is not None:
                finish(*prev)
            old = m_s[at]
            top = largest(parts, old)
            p, total = weigh(parts, top)
            keep = jnp.exp2((old - top) * e)
            prev = p, keep, l_s[at] * keep + total, r, at
        finish(*prev)

    def end_alone():
        for r, at in enumerate(strips):
            share = 1 / jnp.broadcast_to(jnp.sum(l_s[at], axis=1, keepdims=True), (own, 128))
            o_s[:, r * HEAD:(r + 1) * HEAD] = (acc_s[at] * twice(share)).astype(jnp.bfloat16)

    def project(h):
        for t in range(tiles):
            wo_in(h, t).wait()
        for t in range(tiles):
            here = slice(t * tile, (t + 1) * tile)
            y = y_s[:, here] + _dot(o_s[...], wo_s[h, t])
            y_s[:, here] = y
            out_ref[:, here] = y.astype(jnp.bfloat16)

    @pl.when(me == 0)
    def _():
        arrived(1, 1, V)
        push(1, 1, V, L).start()

    def head(h, _):
        first = h == 0

        @pl.when(me <= 1)
        def _():
            begin(h, [me])

        @pl.when(me == 0)
        def _():
            end_alone()

        @pl.when(me == 2)
        def _():
            arrived(1, h, V)
            begin(h, [me, 1])

            @pl.when(first)
            def _():
                arrived(1, 1, K)
                push(1, 1, K, R).start()

            for c in (K, V):
                arrived(0, h, c)

        @pl.when(me == 3)
        def _():
            @pl.when(first)
            def _():
                arrived(0, 0, V)
                push(0, 0, V, L).start()

            @pl.when(jnp.logical_not(first))
            def _():
                for c in (K, V):
                    arrived(0, 1, c)

            for c in (K, V):
                arrived(2, h, c)
            begin(h, [me, 2, 0])
            for c in (K, V):
                arrived(1, h, c)

        @pl.when((me == 1) & first)
        def _():
            for c in (K, V):
                arrived(0, 0, c)

        @pl.when(me >= 1)
        def _():
            end(h, jnp.where(me == 3, 1, 0))

        @pl.when((me == 1) & first)
        def _():
            arrived(0, 1, K)
            push(0, 1, K, R).start()

        project(h)

        @pl.when((me == 1) & first)
        def _():
            arrived(0, 1, V)
            push(0, 1, V, R).start()

    lax.fori_loop(0, kv_heads, head, None)
    wait_sent()


def solution(mesh):
    n = mesh.shape["sp"]

    def step(x, gain, wq, wk, wv, wo):
        own, d = x.shape
        heads, kv_heads = wq.shape[1] // HEAD, wk.shape[1] // HEAD
        per = heads // kv_heads
        tile = 512
        place = np.arange(n * own, dtype=np.float64)[:, None]
        angle = place * THETA ** (-np.arange(HEAD // 2, dtype=np.float64) / (HEAD // 2))
        cos, sin = jnp.asarray(np.cos(angle), jnp.float32), jnp.asarray(np.sin(angle), jnp.float32)
        anywhere = pl.BlockSpec(memory_space=pl.ANY)
        dma = pltpu.SemaphoreType.DMA
        bf16, f32 = jnp.bfloat16, jnp.float32
        return pl.pallas_call(
            functools.partial(_kernel, n=n),
            out_shape=pltpu.VMEM((own, d), bf16),
            in_specs=[anywhere] * 8,
            out_specs=pl.BlockSpec(memory_space=pltpu.VMEM),
            scratch_shapes=[
                pltpu.VMEM((own, d), bf16),
                pltpu.VMEM((d,), bf16),
                pltpu.VMEM((own, HEAD // 2), f32),
                pltpu.VMEM((own, HEAD // 2), f32),
                pltpu.VMEM((kv_heads, d, HEAD), bf16),
                pltpu.VMEM((kv_heads, d, HEAD), bf16),
                pltpu.VMEM((heads, d, HEAD), bf16),
                pltpu.VMEM((kv_heads, d // tile, per * HEAD, tile), bf16),
                pltpu.VMEM((own, d), bf16),
                pltpu.VMEM((kv_heads, per * own, HEAD), bf16),
                pltpu.VMEM((n, kv_heads, 2, own, HEAD), bf16),
                pltpu.VMEM((per * own, HEAD), f32),
                pltpu.VMEM((per * own, 128), f32),
                pltpu.VMEM((per * own, 128), f32),
                pltpu.VMEM((own, per * HEAD), bf16),
                pltpu.VMEM((own, d), f32),
                dma((4,)), dma((kv_heads,)), dma((kv_heads,)), dma((heads,)), dma((kv_heads, d // tile)),
                dma((2, n, kv_heads, 2)), dma((n, kv_heads, 2)),
            ],
            compiler_params=pltpu.CompilerParams(collective_id=0, has_side_effects=True, vmem_limit_bytes=VMEM_LIMIT),
        )(x, gain, cos, sin, wq, wk, wv, wo)

    tokens, whole = P(("dp", "sp"), None), P(None, None)
    return jax.shard_map(
        step,
        mesh=mesh,
        in_specs=(tokens, P(None), whole, whole, whole, whole),
        out_specs=tokens,
        check_vma=False,
    )
```

```python
import functools

import jax
import jax.numpy as jnp
import numpy as np
from jax import lax
from jax.experimental import pallas as pl
from jax.experimental.pallas import tpu as pltpu
from jax.sharding import PartitionSpec as P

HEAD = 256
THETA = 10000
LOG2E = 1.4426950408889634
NEG = -1e30
VMEM_LIMIT = 60 * 2**20
MESH = pl.DeviceIdType.MESH


def _dot(a, b, ca=1, cb=0):
    return lax.dot_general(a, b, (((ca,), (cb,)), ((), ())), preferred_element_type=jnp.float32)


def _kernel(x_hbm, gain_hbm, cos_hbm, sin_hbm, wq_hbm, wk_hbm, wv_hbm, wo_hbm, out_ref,
            x_s, gain_s, cos_s, sin_s, wk_s, wv_s, wq_s, wo_s, a_s, q_s, kv_s, acc_s, m_s, l_s, o_s, y_s,
            in_sem, wk_sem, wv_sem, wq_sem, wo_sem, send_sem, recv_sem, *, n):
    own, d = x_s.shape
    kv_heads, per = q_s.shape[0], q_s.shape[1] // own
    heads = kv_heads * per
    hh = HEAD // 2
    tile = wo_s.shape[3]
    tiles = d // tile
    me = lax.axis_index("sp")
    right, left = lax.rem(me + 1, n), lax.rem(me + n - 1, n)
    K, V = 0, 1

    barrier = pltpu.get_barrier_semaphore()
    for peer in (left, right):
        pl.semaphore_signal(barrier, inc=1, device_id={"sp": peer}, device_id_type=MESH)

    def cols(i, width):
        return pl.ds(i * width if isinstance(i, int) else pl.multiple_of(i * width, width), width)

    x_in = pltpu.make_async_copy(x_hbm, x_s, in_sem.at[0])
    gain_in = pltpu.make_async_copy(gain_hbm, gain_s, in_sem.at[1])
    cos_in = pltpu.make_async_copy(cos_hbm.at[pl.ds(me * own, own)], cos_s, in_sem.at[2])
    sin_in = pltpu.make_async_copy(sin_hbm.at[pl.ds(me * own, own)], sin_s, in_sem.at[3])

    def wk_in(h):
        return pltpu.make_async_copy(wk_hbm.at[:, cols(h, HEAD)], wk_s.at[h], wk_sem.at[h])

    def wv_in(h):
        return pltpu.make_async_copy(wv_hbm.at[:, cols(h, HEAD)], wv_s.at[h], wv_sem.at[h])

    def wq_in(i):
        return pltpu.make_async_copy(wq_hbm.at[:, cols(i, HEAD)], wq_s.at[i], wq_sem.at[i])

    def wo_in(h, t):
        return pltpu.make_async_copy(wo_hbm.at[cols(h, per * HEAD), cols(t, tile)], wo_s.at[h, t], wo_sem.at[h, t])

    x_in.start()
    gain_in.start()
    wk_in(0).start()
    cos_in.start()
    sin_in.start()
    gain_in.wait()
    for h in range(kv_heads):
        if h > 0:
            wk_in(h).start()
        wv_in(h).start()

    x_in.wait()
    for i in range(heads):
        wq_in(i).start(priority=0)
    wide = x_s[...].astype(jnp.float32)
    scale = lax.rsqrt(jnp.mean(wide * wide, -1, keepdims=True) + 1e-6)
    a_s[...] = (wide * scale * gain_s[...].astype(jnp.float32).reshape(1, d)).astype(jnp.bfloat16)

    def turn(t):
        t = t.astype(jnp.bfloat16).astype(jnp.float32)
        a, b = t[:, :hh], t[:, hh:]
        cos, sin = cos_s[...], sin_s[...]
        return (a * cos - b * sin).astype(jnp.bfloat16), (b * cos + a * sin).astype(jnp.bfloat16)

    def push(block, h, c, way):
        return pltpu.make_async_remote_copy(
            src_ref=kv_s.at[block, h, c], dst_ref=kv_s.at[block, h, c], send_sem=send_sem.at[way, block, h, c],
            recv_sem=recv_sem.at[block, h, c], device_id={"sp": left if way else right}, device_id_type=MESH)

    R, L = 0, 1

    def arrived(block, h, c):
        push(block, h, c, R).wait_recv()

    def start_own(h, c):
        @pl.when(me == 0)
        def _():
            push(0, h, c, R).start()
            if h == 0:
                push(0, h, c, L).start()

        @pl.when(me == 1)
        def _():
            push(1, h, c, R).start()
            if c == V:
                push(1, h, c, L).start()

        if h == 0:
            @pl.when(me == 2)
            def _():
                push(2, h, c, R).start()

    def start_later():
        @pl.when(me == 0)
        def _():
            arrived(1, 0, V)
            push(1, 0, V, L).start()
            push(0, 1, K, L).start()
            push(0, 1, V, L).start()

        @pl.when(me == 2)
        def _():
            arrived(1, 0, K)
            push(1, 0, K, R).start()
            push(2, 1, K, R).start()
            push(2, 1, V, R).start()

        @pl.when(me == 3)
        def _():
            arrived(0, 0, K)
            push(0, 0, K, L).start()

    def wait_sent():
        @pl.when(me == 0)
        def _():
            for h in range(kv_heads):
                for c in (K, V):
                    push(0, h, c, R).wait_send()
                    push(0, h, c, L).wait_send()
                push(1, h, V, L).wait_send()

        @pl.when(me == 1)
        def _():
            for h in range(kv_heads):
                for c in (K, V):
                    push(1, h, c, R).wait_send()
                push(1, h, V, L).wait_send()
            for c in (K, V):
                push(0, 1, c, R).wait_send()

        @pl.when(me == 2)
        def _():
            for h in range(kv_heads):
                for c in (K, V):
                    push(2, h, c, R).wait_send()
                push(1, h, K, R).wait_send()

        @pl.when(me == 3)
        def _():
            for c in (K, V):
                push(0, 0, c, L).wait_send()

    for h in range(kv_heads):
        wk_in(h).wait()
        if h == 0:
            cos_in.wait()
            sin_in.wait()
        k1, k2 = turn(_dot(a_s[...], wk_s[h]))
        kv_s[me, h, K, :, :hh] = k1
        kv_s[me, h, K, :, hh:] = k2
        if h == 0:
            pl.semaphore_wait(barrier, 2)
        start_own(h, K)
        wv_in(h).wait()
        kv_s[me, h, V] = _dot(a_s[...], wv_s[h]).astype(jnp.bfloat16)
        start_own(h, V)

    group = 4
    rounds = heads // group

    def query(i, _):
        for r in range(group):
            wq_in(i * group + r).wait()
        for r in range(wo_chunks):
            j = i * wo_chunks + r
            wo_in(lax.div(j, tiles), lax.rem(j, tiles)).start(priority=0)
        for r in range(group):
            j = i * group + r
            q1, q2 = turn(_dot(a_s[...], wq_s[j]))
            rows = pl.ds(pl.multiple_of(lax.rem(j, per) * own, own), own)
            q_s[lax.div(j, per), rows, :hh] = q1
            q_s[lax.div(j, per), rows, hh:] = q2

        @pl.when(i == 1)
        def _():
            start_later()

    wo_chunks = kv_heads * tiles // rounds
    lax.fori_loop(0, rounds, query, None)
    y_s[...] = x_s[...].astype(jnp.float32)

    e = HEAD**-0.5 * LOG2E
    strips = [slice(r * own, (r + 1) * own) for r in range(per)]

    def scores(h, at, blocks, diagonal):
        out = [_dot(q_s[h, at], kv_s[b, h, K], 1, 1) for b in blocks]
        if diagonal:
            seen = lax.broadcasted_iota(jnp.int32, (own, own), 0) >= lax.broadcasted_iota(jnp.int32, (own, own), 1)
            out[0] = jnp.where(seen, out[0], NEG)
        return out

    def largest(parts, old=None):
        top = None
        for s in parts:
            for j in range(0, own, 128):
                top = s[:, j:j + 128] if top is None else jnp.maximum(top, s[:, j:j + 128])
        top = jnp.broadcast_to(jnp.max(top, axis=1, keepdims=True), (own, 128))
        return top if old is None else jnp.maximum(old, top)

    def weigh(parts, top):
        out, total = [], None
        for s in parts:
            for j in range(0, own, 128):
                p = jnp.exp2((s[:, j:j + 128] - top) * e)
                total = p if total is None else total + p
                out.append(p.astype(jnp.bfloat16))
        return jnp.concatenate(out, axis=1), total

    def twice(t):
        return jnp.concatenate([t, t], axis=1)

    def values(h, blocks):
        return jnp.concatenate([kv_s[b, h, V] for b in blocks], axis=0)

    def begin(h, blocks):
        def finish(p, at):
            acc_s[at] = _dot(p, values(h, blocks))

        later, prev = scores(h, strips[0], blocks, True), None
        for r, at in enumerate(strips):
            parts = later
            if r + 1 < per:
                later = scores(h, strips[r + 1], blocks, True)
            if prev is not None:
                finish(*prev)
            top = largest(parts)
            p, total = weigh(parts, top)
            m_s[at] = top
            l_s[at] = total
            prev = p, at
        finish(*prev)

    PIECES = [2, 4, 6, 8]

    def project_piece(h, lo, hi, last):
        for t in range(tiles):
            here = slice(t * tile, (t + 1) * tile)
            y = y_s[:, here] + _dot(o_s[:, lo * HEAD:hi * HEAD], wo_s[h, t, lo * HEAD:hi * HEAD])
            y_s[:, here] = y
            if last:
                out_ref[:, here] = y.astype(jnp.bfloat16)

    def end(h, blocks):
        def finish(p, keep, total, r, at):
            share = 1 / jnp.broadcast_to(jnp.sum(total, axis=1, keepdims=True), (own, 128))
            mix = acc_s[at] * twice(keep) + _dot(p, values(h, blocks))
            o_s[:, r * HEAD:(r + 1) * HEAD] = (mix * twice(share)).astype(jnp.bfloat16)
            if r + 1 in PIECES:
                k = PIECES.index(r + 1)
                project_piece(h, PIECES[k - 1] if k else 0, r + 1, r + 1 == per)

        later, prev = scores(h, strips[0], blocks, False), None
        for r, at in enumerate(strips):
            parts = later
            if r + 1 < per:
                later = scores(h, strips[r + 1], blocks, False)
            if prev is not None:
                finish(*prev)
            old = m_s[at]
            top = largest(parts, old)
            p, total = weigh(parts, top)
            keep = jnp.exp2((old - top) * e)
            prev = p, keep, l_s[at] * keep + total, r, at
        finish(*prev)

    def end_alone():
        for r, at in enumerate(strips):
            share = 1 / jnp.broadcast_to(jnp.sum(l_s[at], axis=1, keepdims=True), (own, 128))
            o_s[:, r * HEAD:(r + 1) * HEAD] = (acc_s[at] * twice(share)).astype(jnp.bfloat16)


    @pl.when(me == 0)
    def _():
        arrived(1, 1, V)
        push(1, 1, V, L).start()

    def head(h, _):
        first = h == 0
        for t in range(tiles):
            wo_in(h, t).wait()

        @pl.when(me <= 1)
        def _():
            begin(h, [me])

        @pl.when(me == 0)
        def _():
            end_alone()
            project_piece(h, 0, per, True)

        @pl.when(me >= 2)
        def _():
            @pl.when((me == 3) & first)
            def _():
                arrived(0, 0, V)
                push(0, 0, V, L).start()

            @pl.when(me == 3)
            def _():
                arrived(2, h, K)

            arrived(me - 1, h, V)
            begin(h, [me, me - 1])

            @pl.when((me == 2) & first)
            def _():
                arrived(1, 1, K)
                push(1, 1, K, R).start()

            @pl.when((me == 2) | jnp.logical_not(first))
            def _():
                for c in (K, V):
                    arrived(0, h, c)

        @pl.when(me == 3)
        def _():
            for c in (K, V):
                arrived(1, h, c)
            end(h, [0, 1])

        @pl.when((me == 1) & first)
        def _():
            for c in (K, V):
                arrived(0, 0, c)
            arrived(0, 1, K)
            push(0, 1, K, R).start()

        @pl.when((me == 1) | (me == 2))
        def _():
            end(h, [0])


        @pl.when((me == 1) & first)
        def _():
            arrived(0, 1, V)
            push(0, 1, V, R).start()

    lax.fori_loop(0, kv_heads, head, None)
    wait_sent()


def solution(mesh):
    n = mesh.shape["sp"]

    def step(x, gain, wq, wk, wv, wo):
        own, d = x.shape
        heads, kv_heads = wq.shape[1] // HEAD, wk.shape[1] // HEAD
        per = heads // kv_heads
        tile = 512
        place = np.arange(n * own, dtype=np.float64)[:, None]
        angle = place * THETA ** (-np.arange(HEAD // 2, dtype=np.float64) / (HEAD // 2))
        cos, sin = jnp.asarray(np.cos(angle), jnp.float32), jnp.asarray(np.sin(angle), jnp.float32)
        anywhere = pl.BlockSpec(memory_space=pl.ANY)
        dma = pltpu.SemaphoreType.DMA
        bf16, f32 = jnp.bfloat16, jnp.float32
        return pl.pallas_call(
            functools.partial(_kernel, n=n),
            out_shape=pltpu.VMEM((own, d), bf16),
            in_specs=[anywhere] * 8,
            out_specs=pl.BlockSpec(memory_space=pltpu.VMEM),
            scratch_shapes=[
                pltpu.VMEM((own, d), bf16),
                pltpu.VMEM((d,), bf16),
                pltpu.VMEM((own, HEAD // 2), f32),
                pltpu.VMEM((own, HEAD // 2), f32),
                pltpu.VMEM((kv_heads, d, HEAD), bf16),
                pltpu.VMEM((kv_heads, d, HEAD), bf16),
                pltpu.VMEM((heads, d, HEAD), bf16),
                pltpu.VMEM((kv_heads, d // tile, per * HEAD, tile), bf16),
                pltpu.VMEM((own, d), bf16),
                pltpu.VMEM((kv_heads, per * own, HEAD), bf16),
                pltpu.VMEM((n, kv_heads, 2, own, HEAD), bf16),
                pltpu.VMEM((per * own, HEAD), f32),
                pltpu.VMEM((per * own, 128), f32),
                pltpu.VMEM((per * own, 128), f32),
                pltpu.VMEM((own, per * HEAD), bf16),
                pltpu.VMEM((own, d), f32),
                dma((4,)), dma((kv_heads,)), dma((kv_heads,)), dma((heads,)), dma((kv_heads, d // tile)),
                dma((2, n, kv_heads, 2)), dma((n, kv_heads, 2)),
            ],
            compiler_params=pltpu.CompilerParams(collective_id=0, has_side_effects=True, vmem_limit_bytes=VMEM_LIMIT),
        )(x, gain, cos, sin, wq, wk, wv, wo)

    tokens, whole = P(("dp", "sp"), None), P(None, None)
    return jax.shard_map(
        step,
        mesh=mesh,
        in_specs=(tokens, P(None), whole, whole, whole, whole),
        out_specs=tokens,
        check_vma=False,
    )
```

```python
import functools

import jax
import jax.numpy as jnp
import numpy as np
from jax import lax
from jax.experimental import pallas as pl
from jax.experimental.pallas import tpu as pltpu
from jax.sharding import PartitionSpec as P

HEAD = 256
THETA = 10000
LOG2E = 1.4426950408889634
NEG = -1e30
VMEM_LIMIT = 52 * 2**20
LAST_LIMIT = 8 * 2**20
MESH = pl.DeviceIdType.MESH


def _dot(a, b, ca=1, cb=0):
    return lax.dot_general(a, b, (((ca,), (cb,)), ((), ())), preferred_element_type=jnp.float32)


def _kernel(x_hbm, gain_hbm, cos_hbm, sin_hbm, wq_hbm, wk_hbm, wv_hbm, wo_hbm, o_s, y_s, wo_last,
            x_s, gain_s, cos_s, sin_s, wk_s, wv_s, wq_s, wo_s, a_s, q_s, kv_s, acc_s, m_s, l_s, p_s,
            in_sem, wk_sem, wv_sem, wq_sem, wo_sem, send_sem, recv_sem, *, n):
    own, d = x_s.shape
    kv_heads, per = q_s.shape[0], q_s.shape[1] // own
    heads = kv_heads * per
    hh = HEAD // 2
    tile = wo_s.shape[2]
    tiles = d // tile
    me = lax.axis_index("sp")
    right, left = lax.rem(me + 1, n), lax.rem(me + n - 1, n)
    K, V = 0, 1

    barrier = pltpu.get_barrier_semaphore()
    for peer in (left, right):
        pl.semaphore_signal(barrier, inc=1, device_id={"sp": peer}, device_id_type=MESH)

    def cols(i, width):
        return pl.ds(i * width if isinstance(i, int) else pl.multiple_of(i * width, width), width)

    x_in = pltpu.make_async_copy(x_hbm, x_s, in_sem.at[0])
    gain_in = pltpu.make_async_copy(gain_hbm, gain_s, in_sem.at[1])
    cos_in = pltpu.make_async_copy(cos_hbm.at[pl.ds(me * own, own)], cos_s, in_sem.at[2])
    sin_in = pltpu.make_async_copy(sin_hbm.at[pl.ds(me * own, own)], sin_s, in_sem.at[3])

    def wk_in(h):
        return pltpu.make_async_copy(wk_hbm.at[:, cols(h, HEAD)], wk_s.at[h], wk_sem.at[h])

    def wv_in(h):
        return pltpu.make_async_copy(wv_hbm.at[:, cols(h, HEAD)], wv_s.at[h], wv_sem.at[h])

    def wq_in(i):
        return pltpu.make_async_copy(wq_hbm.at[:, cols(i, HEAD)], wq_s.at[i], wq_sem.at[i])

    def wo_in(h, t):
        return pltpu.make_async_copy(wo_hbm.at[cols(h, per * HEAD), cols(t, tile)], (wo_last if h else wo_s).at[t], wo_sem.at[h, t])

    x_in.start()
    gain_in.start()
    wk_in(0).start()
    cos_in.start()
    sin_in.start()
    gain_in.wait()
    for h in range(kv_heads):
        if h > 0:
            wk_in(h).start()
        wv_in(h).start()

    x_in.wait()
    for i in range(heads):
        wq_in(i).start(priority=0)
    wide = x_s[...].astype(jnp.float32)
    scale = lax.rsqrt(jnp.mean(wide * wide, -1, keepdims=True) + 1e-6)
    a_s[...] = (wide * scale * gain_s[...].astype(jnp.float32).reshape(1, d)).astype(jnp.bfloat16)

    def turn(t):
        t = t.astype(jnp.bfloat16).astype(jnp.float32)
        a, b = t[:, :hh], t[:, hh:]
        cos, sin = cos_s[...], sin_s[...]
        return (a * cos - b * sin).astype(jnp.bfloat16), (b * cos + a * sin).astype(jnp.bfloat16)

    def push(block, h, c, way):
        return pltpu.make_async_remote_copy(
            src_ref=kv_s.at[block, h, c], dst_ref=kv_s.at[block, h, c], send_sem=send_sem.at[way, block, h, c],
            recv_sem=recv_sem.at[block, h, c], device_id={"sp": left if way else right}, device_id_type=MESH)

    R, L = 0, 1

    def arrived(block, h, c):
        push(block, h, c, R).wait_recv()

    def start_own(h, c):
        @pl.when(me == 0)
        def _():
            push(0, h, c, R).start()
            if h == 0:
                push(0, h, c, L).start()

        @pl.when(me == 1)
        def _():
            push(1, h, c, R).start()
            if c == V:
                push(1, h, c, L).start()

        if h == 0:
            @pl.when(me == 2)
            def _():
                push(2, h, c, R).start()

    def start_later():
        @pl.when(me == 0)
        def _():
            arrived(1, 0, V)
            push(1, 0, V, L).start()
            push(0, 1, K, L).start()
            push(0, 1, V, L).start()

        @pl.when(me == 2)
        def _():
            arrived(1, 0, K)
            push(1, 0, K, R).start()
            push(2, 1, K, R).start()

        @pl.when(me == 3)
        def _():
            arrived(0, 0, K)
            push(0, 0, K, L).start()

    def wait_sent():
        @pl.when(me == 0)
        def _():
            for h in range(kv_heads):
                for c in (K, V):
                    push(0, h, c, R).wait_send()
                    push(0, h, c, L).wait_send()
                push(1, h, V, L).wait_send()

        @pl.when(me == 1)
        def _():
            for h in range(kv_heads):
                for c in (K, V):
                    push(1, h, c, R).wait_send()
                push(1, h, V, L).wait_send()
            for c in (K, V):
                push(0, 1, c, R).wait_send()

        @pl.when(me == 2)
        def _():
            for h in range(kv_heads):
                for c in (K, V):
                    push(2, h, c, R).wait_send()
                push(1, h, K, R).wait_send()

        @pl.when(me == 3)
        def _():
            for c in (K, V):
                push(0, 0, c, L).wait_send()

    for h in range(kv_heads):
        wk_in(h).wait()
        if h == 0:
            cos_in.wait()
            sin_in.wait()
        k1, k2 = turn(_dot(a_s[...], wk_s[h]))
        kv_s[me, h, K, :, :hh] = k1
        kv_s[me, h, K, :, hh:] = k2
        if h == 0:
            pl.semaphore_wait(barrier, 2)
        start_own(h, K)
        wv_in(h).wait()
        kv_s[me, h, V] = _dot(a_s[...], wv_s[h]).astype(jnp.bfloat16)
        start_own(h, V)

    group = 4
    rounds = heads // group

    def query(i, _):
        for r in range(group):
            wq_in(i * group + r).wait()
        for h in range(kv_heads):
            for r in range(wo_chunks):
                @pl.when(lax.div(i * kv_heads, rounds) == h)
                def _():
                    wo_in(h, lax.rem(i * wo_chunks + r, tiles)).start()

        for r in range(group):
            j = i * group + r
            q1, q2 = turn(_dot(a_s[...], wq_s[j]))
            rows = pl.ds(pl.multiple_of(lax.rem(j, per) * own, own), own)
            q_s[lax.div(j, per), rows, :hh] = q1
            q_s[lax.div(j, per), rows, hh:] = q2

        @pl.when(i == 1)
        def _():
            start_later()

    wo_chunks = kv_heads * tiles // rounds
    lax.fori_loop(0, rounds, query, None)
    y_s[...] = x_s[...].astype(jnp.float32)

    e = HEAD**-0.5 * LOG2E
    strips = [slice(r * own, (r + 1) * own) for r in range(per)]

    def scores(h, at, blocks, diagonal):
        out = [_dot(q_s[h, at], kv_s[b, h, K], 1, 1) for b in blocks]
        if diagonal:
            seen = lax.broadcasted_iota(jnp.int32, (own, own), 0) >= lax.broadcasted_iota(jnp.int32, (own, own), 1)
            out[0] = jnp.where(seen, out[0], NEG)
        return out

    def largest(parts, old=None):
        top = None
        for s in parts:
            for j in range(0, own, 128):
                top = s[:, j:j + 128] if top is None else jnp.maximum(top, s[:, j:j + 128])
        top = jnp.broadcast_to(jnp.max(top, axis=1, keepdims=True), (own, 128))
        return top if old is None else jnp.maximum(old, top)

    def weigh(parts, top):
        out, total = [], None
        for s in parts:
            for j in range(0, own, 128):
                p = jnp.exp2((s[:, j:j + 128] - top) * e)
                total = p if total is None else total + p
                out.append(p.astype(jnp.bfloat16))
        return jnp.concatenate(out, axis=1), total

    def twice(t):
        return jnp.concatenate([t, t], axis=1)

    def values(h, blocks):
        return jnp.concatenate([kv_s[b, h, V] for b in blocks], axis=0)

    def begin(h, blocks):
        def finish(p, at):
            acc_s[h, at] = _dot(p, values(h, blocks))

        later, prev = scores(h, strips[0], blocks, True), None
        for r, at in enumerate(strips):
            parts = later
            if r + 1 < per:
                later = scores(h, strips[r + 1], blocks, True)
            if prev is not None:
                finish(*prev)
            top = largest(parts)
            p, total = weigh(parts, top)
            m_s[h, at] = top
            l_s[h, at] = total
            prev = p, at
        finish(*prev)

    def project():
        for t in range(tiles):
            here = slice(t * tile, (t + 1) * tile)
            y_s[:, here] = y_s[:, here] + _dot(o_s[...], wo_s[t])

    def result(p, keep, total, h, blocks, r, at):
        share = 1 / jnp.broadcast_to(jnp.sum(total, axis=1, keepdims=True), (own, 128))
        mix = acc_s[h, at] * twice(keep) + _dot(p, values(h, blocks))
        o_s[:, r * HEAD:(r + 1) * HEAD] = (mix * twice(share)).astype(jnp.bfloat16)

    def rest(h, blocks, use):
        later = scores(h, strips[0], blocks, False)
        for r, at in enumerate(strips):
            parts = later
            if r + 1 < per:
                later = scores(h, strips[r + 1], blocks, False)
            old = m_s[h, at]
            top = largest(parts, old)
            p, total = weigh(parts, top)
            keep = jnp.exp2((old - top) * e)
            use(p, keep, l_s[h, at] * keep + total, r, at)
        use(None, None, None, per, None)

    def end(h, blocks):
        held = []

        def use(p, keep, total, r, at):
            if held:
                result(*held.pop())
            held.append((p, keep, total, h, blocks, r, at))

        rest(h, blocks, use)

    def weigh_rest(h, blocks):
        def use(p, keep, total, r, at):
            if r < per:
                p_s[at, :len(blocks) * own] = p
                m_s[h, at] = keep
                l_s[h, at] = total

        rest(h, blocks, use)

    def end_rest(h, blocks):
        for r, at in enumerate(strips):
            result(p_s[at, :len(blocks) * own], m_s[h, at], l_s[h, at], h, blocks, r, at)

    def end_alone(h):
        for r, at in enumerate(strips):
            share = 1 / jnp.broadcast_to(jnp.sum(l_s[h, at], axis=1, keepdims=True), (own, 128))
            o_s[:, r * HEAD:(r + 1) * HEAD] = (acc_s[h, at] * twice(share)).astype(jnp.bfloat16)


    @pl.when(me == 0)
    def _():
        arrived(1, 1, V)
        push(1, 1, V, L).start()

    def head(h, _):
        first, second = h == 0, h > 0

        @pl.when((me == 3) & first)
        def _():
            arrived(0, 0, V)
            push(0, 0, V, L).start()
            arrived(2, 0, K)

        @pl.when((me >= 2) & first)
        def _():
            arrived(me - 1, 0, V)
            begin(0, [me, me - 1])

        @pl.when((me <= 1) | first)
        def _():
            begin(jnp.where(me <= 1, h, 1), [me])

        @pl.when(me == 0)
        def _():
            end_alone(h)

        @pl.when((me == 1) & first)
        def _():
            for c in (K, V):
                arrived(0, 0, c)
            arrived(0, 1, K)
            push(0, 1, K, R).start()

        @pl.when((me == 2) & first)
        def _():
            arrived(1, 1, K)
            push(1, 1, K, R).start()
            push(2, 1, V, R).start()
            for c in (K, V):
                arrived(0, 0, c)

        @pl.when((me == 1) | ((me == 2) & first))
        def _():
            end(h, [0])

        @pl.when((me == 1) & first)
        def _():
            arrived(0, 1, V)
            push(0, 1, V, R).start()

        @pl.when((me == 3) & first)
        def _():
            for c in (K, V):
                arrived(1, 0, c)
            end(h, [0, 1])

        @pl.when((me == 2) & second)
        def _():
            arrived(0, 1, K)
            weigh_rest(1, [1, 0])
            arrived(1, 1, V)
            arrived(0, 1, V)
            end_rest(1, [1, 0])

        @pl.when((me == 3) & second)
        def _():
            others = [0, 2, 1]
            for b in others:
                arrived(b, 1, K)
            weigh_rest(1, others)
            for b in others:
                arrived(b, 1, V)
            end_rest(1, others)

        @pl.when(first)
        def _():
            for t in range(tiles):
                wo_in(0, t).wait()
            project()

    lax.fori_loop(0, kv_heads, head, None)
    for t in range(tiles):
        wo_in(1, t).wait()
    wait_sent()


def _last(o_ref, y_ref, w_ref, out_hbm, out_s, sem):
    tiles, _, tile = w_ref.shape
    step = min(tile, HEAD)
    per = tile // step

    def leave(i):
        return pltpu.make_async_copy(out_s.at[:, i * step:(i + 1) * step], out_hbm.at[:, i * step:(i + 1) * step], sem.at[i])

    for i in range(tiles * per):
        here = slice(i * step, (i + 1) * step)
        w = w_ref[i // per, :, (i % per) * step:(i % per + 1) * step]
        out_s[:, here] = (y_ref[:, here] + _dot(o_ref[...], w)).astype(out_s.dtype)
        leave(i).start()
    for i in range(tiles * per):
        leave(i).wait()


def solution(mesh):
    n = mesh.shape["sp"]

    def step(x, gain, wq, wk, wv, wo):
        own, d = x.shape
        heads, kv_heads = wq.shape[1] // HEAD, wk.shape[1] // HEAD
        per = heads // kv_heads
        tile = 512
        place = np.arange(n * own, dtype=np.float64)[:, None]
        angle = place * THETA ** (-np.arange(HEAD // 2, dtype=np.float64) / (HEAD // 2))
        cos, sin = jnp.asarray(np.cos(angle), jnp.float32), jnp.asarray(np.sin(angle), jnp.float32)
        anywhere = pl.BlockSpec(memory_space=pl.ANY)
        dma = pltpu.SemaphoreType.DMA
        bf16, f32 = jnp.bfloat16, jnp.float32
        vmem = pl.BlockSpec(memory_space=pltpu.VMEM)
        o, y, w = pl.pallas_call(
            functools.partial(_kernel, n=n),
            out_shape=[pltpu.VMEM((own, per * HEAD), bf16), pltpu.VMEM((own, d), f32), pltpu.VMEM((d // tile, per * HEAD, tile), bf16)],
            in_specs=[anywhere] * 8,
            out_specs=[vmem] * 3,
            scratch_shapes=[
                pltpu.VMEM((own, d), bf16),
                pltpu.VMEM((d,), bf16),
                pltpu.VMEM((own, HEAD // 2), f32),
                pltpu.VMEM((own, HEAD // 2), f32),
                pltpu.VMEM((kv_heads, d, HEAD), bf16),
                pltpu.VMEM((kv_heads, d, HEAD), bf16),
                pltpu.VMEM((heads, d, HEAD), bf16),
                pltpu.VMEM((d // tile, per * HEAD, tile), bf16),
                pltpu.VMEM((own, d), bf16),
                pltpu.VMEM((kv_heads, per * own, HEAD), bf16),
                pltpu.VMEM((n, kv_heads, 2, own, HEAD), bf16),
                pltpu.VMEM((kv_heads, per * own, HEAD), f32),
                pltpu.VMEM((kv_heads, per * own, 128), f32),
                pltpu.VMEM((kv_heads, per * own, 128), f32),
                pltpu.VMEM((per * own, (n - 1) * own), bf16),
                dma((4,)), dma((kv_heads,)), dma((kv_heads,)), dma((heads,)), dma((kv_heads, d // tile)),
                dma((2, n, kv_heads, 2)), dma((n, kv_heads, 2)),
            ],
            compiler_params=pltpu.CompilerParams(collective_id=0, has_side_effects=True, vmem_limit_bytes=VMEM_LIMIT),
        )(x, gain, cos, sin, wq, wk, wv, wo)
        return pl.pallas_call(
            _last,
            out_shape=jax.ShapeDtypeStruct((own, d), bf16),
            in_specs=[vmem] * 3,
            out_specs=anywhere,
            scratch_shapes=[pltpu.VMEM((own, d), bf16), dma((d // min(tile, HEAD),))],
            compiler_params=pltpu.CompilerParams(vmem_limit_bytes=LAST_LIMIT),
        )(o, y, w)

    tokens, whole = P(("dp", "sp"), None), P(None, None)
    return jax.shard_map(
        step,
        mesh=mesh,
        in_specs=(tokens, P(None), whole, whole, whole, whole),
        out_specs=tokens,
        check_vma=False,
    )
```

```python
import functools

import jax
import jax.numpy as jnp
import numpy as np
from jax import lax
from jax.experimental import pallas as pl
from jax.experimental.pallas import tpu as pltpu
from jax.sharding import PartitionSpec as P

HEAD = 256
THETA = 10000
LOG2E = 1.4426950408889634
NEG = -1e30
VMEM_LIMIT = 52 * 2**20
LAST_LIMIT = 8 * 2**20
MESH = pl.DeviceIdType.MESH


def _dot(a, b, ca=1, cb=0):
    return lax.dot_general(a, b, (((ca,), (cb,)), ((), ())), preferred_element_type=jnp.float32)


def _kernel(x_hbm, gain_hbm, turn_hbm, wq_hbm, wk_hbm, wv_hbm, wo_hbm, o_s, y_s, wo_last,
            x_s, gain_s, turn_s, wk_s, wv_s, wq_s, wo_s, a_s, q_s, kv_s, acc_s, m_s, l_s, p_s,
            in_sem, wk_sem, wv_sem, wq_sem, wo_sem, send_sem, recv_sem, *, n):
    own, d = x_s.shape
    kv_heads, per = q_s.shape[0], q_s.shape[1] // own
    heads = kv_heads * per
    hh = HEAD // 2
    rounds, wide_q = wq_s.shape[0], wq_s.shape[2]
    group = wide_q // HEAD
    tile = 512
    tiles = d // tile
    me = lax.axis_index("sp")
    right, left = lax.rem(me + 1, n), lax.rem(me + n - 1, n)
    K, V = 0, 1
    R, L = 0, 1

    barrier = pltpu.get_barrier_semaphore()
    for peer in (left, right):
        pl.semaphore_signal(barrier, inc=1, device_id={"sp": peer}, device_id_type=MESH)

    def cols(i, width):
        return pl.ds(i * width if isinstance(i, int) else pl.multiple_of(i * width, width), width)

    x_in = pltpu.make_async_copy(x_hbm, x_s, in_sem.at[0])
    gain_in = pltpu.make_async_copy(gain_hbm, gain_s, in_sem.at[1])
    turn_in = pltpu.make_async_copy(turn_hbm.at[pl.ds(me * own, own)], turn_s, in_sem.at[2])

    def wk_in(h):
        return pltpu.make_async_copy(wk_hbm.at[:, cols(h, HEAD)], wk_s.at[h], wk_sem.at[h])

    def wv_in(h):
        return pltpu.make_async_copy(wv_hbm.at[:, cols(h, HEAD)], wv_s.at[h], wv_sem.at[h])

    def wq_in(i):
        return pltpu.make_async_copy(wq_hbm.at[:, cols(i, wide_q)], wq_s.at[i], wq_sem.at[i])

    def wo_in(h):
        return pltpu.make_async_copy(wo_hbm.at[cols(h, per * HEAD)], wo_last if h else wo_s, wo_sem.at[h])

    x_in.start()
    gain_in.start()
    wk_in(0).start()
    turn_in.start()
    gain_in.wait()
    for h in range(kv_heads):
        if h > 0:
            wk_in(h).start()
        wv_in(h).start()

    x_in.wait()
    for i in range(rounds):
        wq_in(i).start()
    wide = x_s[...].astype(jnp.float32)
    scale = lax.rsqrt(jnp.mean(wide * wide, -1, keepdims=True) + 1e-6)
    a_s[...] = (wide * scale * gain_s[...].astype(jnp.float32).reshape(1, d)).astype(jnp.bfloat16)

    def turn(t):
        t = t.astype(jnp.bfloat16).astype(jnp.float32)
        a, b = t[:, :hh], t[:, hh:]
        cos, sin = turn_s[:, :hh], turn_s[:, hh:]
        return (a * cos - b * sin).astype(jnp.bfloat16), (b * cos + a * sin).astype(jnp.bfloat16)

    def push(block, h, c, way):
        place = (block * kv_heads + h) * 2 + c
        out = place if way == R else (n - 1) * kv_heads * 2 + (h * 2 + c if block == 0 else kv_heads * 2 + h)
        return pltpu.make_async_remote_copy(
            src_ref=kv_s.at[block, h, c], dst_ref=kv_s.at[block, h, c], send_sem=send_sem.at[out],
            recv_sem=recv_sem.at[place], device_id={"sp": left if way else right}, device_id_type=MESH)

    def arrived(block, h, c):
        push(block, h, c, R).wait_recv()

    def start_own(h, c):
        @pl.when(me == 0)
        def _():
            push(0, h, c, R).start()
            if h == 0:
                push(0, h, c, L).start()

        @pl.when(me == 1)
        def _():
            push(1, h, c, R).start()
            if c == V:
                push(1, h, c, L).start()

        if h == 0:
            @pl.when(me == 2)
            def _():
                push(2, h, c, R).start()

    def start_later():
        @pl.when(me == 0)
        def _():
            arrived(1, 0, V)
            push(1, 0, V, L).start()
            push(0, 1, K, L).start()
            push(0, 1, V, L).start()

        @pl.when(me == 2)
        def _():
            arrived(1, 0, K)
            push(1, 0, K, R).start()
            push(2, 1, K, R).start()

        @pl.when(me == 3)
        def _():
            arrived(0, 0, K)
            push(0, 0, K, L).start()

    def wait_sent():
        @pl.when(me == 0)
        def _():
            for h in range(kv_heads):
                for c in (K, V):
                    push(0, h, c, R).wait_send()
                    push(0, h, c, L).wait_send()
                push(1, h, V, L).wait_send()

        @pl.when(me == 1)
        def _():
            for h in range(kv_heads):
                for c in (K, V):
                    push(1, h, c, R).wait_send()
                push(1, h, V, L).wait_send()
            for c in (K, V):
                push(0, 1, c, R).wait_send()

        @pl.when(me == 2)
        def _():
            for h in range(kv_heads):
                for c in (K, V):
                    push(2, h, c, R).wait_send()
                push(1, h, K, R).wait_send()

        @pl.when(me == 3)
        def _():
            for c in (K, V):
                push(0, 0, c, L).wait_send()

    for h in range(kv_heads):
        wk_in(h).wait()
        if h == 0:
            turn_in.wait()
        k1, k2 = turn(_dot(a_s[...], wk_s[h]))
        kv_s[me, h, K, :, :hh] = k1
        kv_s[me, h, K, :, hh:] = k2
        if h == 0:
            pl.semaphore_wait(barrier, 2)
        start_own(h, K)
        wv_in(h).wait()
        kv_s[me, h, V] = _dot(a_s[...], wv_s[h]).astype(jnp.bfloat16)
        start_own(h, V)


    def query(i, _):
        wq_in(i).wait()
        for h in range(kv_heads):
            @pl.when(i == 1 + h)
            def _():
                wo_in(h).start()

        for r in range(group):
            j = i * group + r
            q1, q2 = turn(_dot(a_s[...], wq_s[i, :, r * HEAD:(r + 1) * HEAD]))
            rows = pl.ds(pl.multiple_of(lax.rem(j, per) * own, own), own)
            q_s[lax.div(j, per), rows, :hh] = q1
            q_s[lax.div(j, per), rows, hh:] = q2

        @pl.when(i == 1)
        def _():
            start_later()

    lax.fori_loop(0, rounds, query, None)
    y_s[...] = x_s[...].astype(jnp.float32)

    e = HEAD**-0.5 * LOG2E
    strips = [slice(r * own, (r + 1) * own) for r in range(per)]

    def scores(h, at, blocks, diagonal):
        out = [_dot(q_s[h, at], kv_s[b, h, K], 1, 1) for b in blocks]
        if diagonal:
            seen = lax.broadcasted_iota(jnp.int32, (own, own), 0) >= lax.broadcasted_iota(jnp.int32, (own, own), 1)
            out[0] = jnp.where(seen, out[0], NEG)
        return out

    def largest(parts, old=None):
        top = None
        for s in parts:
            for j in range(0, own, 128):
                top = s[:, j:j + 128] if top is None else jnp.maximum(top, s[:, j:j + 128])
        top = jnp.broadcast_to(jnp.max(top, axis=1, keepdims=True), (own, 128))
        return top if old is None else jnp.maximum(old, top)

    def weigh(parts, top):
        out, total = [], None
        for s in parts:
            for j in range(0, own, 128):
                p = jnp.exp2((s[:, j:j + 128] - top) * e)
                total = p if total is None else total + p
                out.append(p.astype(jnp.bfloat16))
        return jnp.concatenate(out, axis=1), total

    def twice(t):
        return jnp.concatenate([t, t], axis=1)

    def values(h, blocks):
        return jnp.concatenate([kv_s[b, h, V] for b in blocks], axis=0)

    def begin(h, blocks):
        def finish(p, at):
            acc_s[h, at] = _dot(p, values(h, blocks))

        later, prev = scores(h, strips[0], blocks, True), None
        for r, at in enumerate(strips):
            parts = later
            if r + 1 < per:
                later = scores(h, strips[r + 1], blocks, True)
            if prev is not None:
                finish(*prev)
            top = largest(parts)
            p, total = weigh(parts, top)
            m_s[h, at] = top
            l_s[h, at] = total
            prev = p, at
        finish(*prev)

    def project():
        for t in range(tiles):
            here = slice(t * tile, (t + 1) * tile)
            y_s[:, here] = y_s[:, here] + _dot(o_s[...], wo_s[:, here])

    def result(p, keep, total, h, blocks, r, at):
        share = 1 / jnp.broadcast_to(jnp.sum(total, axis=1, keepdims=True), (own, 128))
        mix = acc_s[h, at] * twice(keep) + _dot(p, values(h, blocks))
        o_s[:, r * HEAD:(r + 1) * HEAD] = (mix * twice(share)).astype(jnp.bfloat16)

    def rest(h, blocks, use):
        later = scores(h, strips[0], blocks, False)
        for r, at in enumerate(strips):
            parts = later
            if r + 1 < per:
                later = scores(h, strips[r + 1], blocks, False)
            old = m_s[h, at]
            top = largest(parts, old)
            p, total = weigh(parts, top)
            keep = jnp.exp2((old - top) * e)
            use(p, keep, l_s[h, at] * keep + total, r, at)
        use(None, None, None, per, None)

    def end(h, blocks):
        held = []

        def use(p, keep, total, r, at):
            if held:
                result(*held.pop())
            held.append((p, keep, total, h, blocks, r, at))

        rest(h, blocks, use)

    def weigh_rest(h, blocks):
        def use(p, keep, total, r, at):
            if r < per:
                p_s[at, :len(blocks) * own] = p
                m_s[h, at] = keep
                l_s[h, at] = total

        rest(h, blocks, use)

    def end_rest(h, blocks):
        for r, at in enumerate(strips):
            result(p_s[at, :len(blocks) * own], m_s[h, at], l_s[h, at], h, blocks, r, at)

    def end_alone(h):
        for r, at in enumerate(strips):
            share = 1 / jnp.broadcast_to(jnp.sum(l_s[h, at], axis=1, keepdims=True), (own, 128))
            o_s[:, r * HEAD:(r + 1) * HEAD] = (acc_s[h, at] * twice(share)).astype(jnp.bfloat16)


    @pl.when(me == 0)
    def _():
        arrived(1, 1, V)
        push(1, 1, V, L).start()

    def head(h, _):
        first, second = h == 0, h > 0

        @pl.when((me == 3) & first)
        def _():
            arrived(0, 0, V)
            push(0, 0, V, L).start()
            arrived(2, 0, K)

        @pl.when((me >= 2) & first)
        def _():
            arrived(me - 1, 0, V)
            begin(0, [me, me - 1])

        @pl.when((me <= 1) | first)
        def _():
            begin(jnp.where(me <= 1, h, 1), [me])

        @pl.when(me == 0)
        def _():
            end_alone(h)

        @pl.when((me == 1) & first)
        def _():
            for c in (K, V):
                arrived(0, 0, c)
            arrived(0, 1, K)
            push(0, 1, K, R).start()

        @pl.when((me == 2) & first)
        def _():
            arrived(1, 1, K)
            push(1, 1, K, R).start()
            push(2, 1, V, R).start()
            for c in (K, V):
                arrived(0, 0, c)

        @pl.when((me == 1) | ((me == 2) & first))
        def _():
            end(h, [0])

        @pl.when((me == 1) & first)
        def _():
            arrived(0, 1, V)
            push(0, 1, V, R).start()

        @pl.when((me == 3) & first)
        def _():
            for c in (K, V):
                arrived(1, 0, c)
            end(h, [0, 1])

        @pl.when((me == 2) & second)
        def _():
            arrived(0, 1, K)
            weigh_rest(1, [1, 0])
            arrived(1, 1, V)
            arrived(0, 1, V)
            end_rest(1, [1, 0])

        @pl.when((me == 3) & second)
        def _():
            others = [0, 2, 1]
            for b in others:
                arrived(b, 1, K)
            weigh_rest(1, others)
            for b in others:
                arrived(b, 1, V)
            end_rest(1, others)

        @pl.when(first)
        def _():
            wo_in(0).wait()
            project()

    lax.fori_loop(0, kv_heads, head, None)
    wo_in(1).wait()
    wait_sent()


def _last(o_ref, y_ref, w_ref, out_hbm, out_s, sem):
    tiles = sem.shape[0]
    tile = out_s.shape[1] // tiles

    def leave(i):
        here = slice(i * tile, (i + 1) * tile)
        return pltpu.make_async_copy(out_s.at[:, here], out_hbm.at[:, here], sem.at[i])

    for i in range(tiles):
        here = slice(i * tile, (i + 1) * tile)
        out_s[:, here] = (y_ref[:, here] + _dot(o_ref[...], w_ref[:, here])).astype(out_s.dtype)
        leave(i).start()
    for i in range(tiles):
        leave(i).wait()


def solution(mesh):
    n = mesh.shape["sp"]

    def step(x, gain, wq, wk, wv, wo):
        own, d = x.shape
        heads, kv_heads = wq.shape[1] // HEAD, wk.shape[1] // HEAD
        per = heads // kv_heads
        tile, wide_q = 512, 1024
        place = np.arange(n * own, dtype=np.float64)[:, None]
        angle = place * THETA ** (-np.arange(HEAD // 2, dtype=np.float64) / (HEAD // 2))
        table = jnp.asarray(np.concatenate([np.cos(angle), np.sin(angle)], 1), jnp.float32)
        anywhere = pl.BlockSpec(memory_space=pl.ANY)
        dma = pltpu.SemaphoreType.DMA
        bf16, f32 = jnp.bfloat16, jnp.float32
        vmem = pl.BlockSpec(memory_space=pltpu.VMEM)
        o, y, w = pl.pallas_call(
            functools.partial(_kernel, n=n),
            out_shape=[pltpu.VMEM((own, per * HEAD), bf16), pltpu.VMEM((own, d), f32), pltpu.VMEM((per * HEAD, d), bf16)],
            in_specs=[anywhere] * 7,
            out_specs=[vmem] * 3,
            scratch_shapes=[
                pltpu.VMEM((own, d), bf16),
                pltpu.VMEM((d,), bf16),
                pltpu.VMEM((own, HEAD), f32),
                pltpu.VMEM((kv_heads, d, HEAD), bf16),
                pltpu.VMEM((kv_heads, d, HEAD), bf16),
                pltpu.VMEM((heads * HEAD // wide_q, d, wide_q), bf16),
                pltpu.VMEM((per * HEAD, d), bf16),
                pltpu.VMEM((own, d), bf16),
                pltpu.VMEM((kv_heads, per * own, HEAD), bf16),
                pltpu.VMEM((n, kv_heads, 2, own, HEAD), bf16),
                pltpu.VMEM((kv_heads, per * own, HEAD), f32),
                pltpu.VMEM((kv_heads, per * own, 128), f32),
                pltpu.VMEM((kv_heads, per * own, 128), f32),
                pltpu.VMEM((per * own, (n - 1) * own), bf16),
                dma((3,)), dma((kv_heads,)), dma((kv_heads,)), dma((heads * HEAD // wide_q,)), dma((kv_heads,)),
                dma(((n - 1) * kv_heads * 2 + kv_heads * 3,)), dma(((n - 1) * kv_heads * 2,)),
            ],
            compiler_params=pltpu.CompilerParams(collective_id=0, has_side_effects=True, vmem_limit_bytes=VMEM_LIMIT),
        )(x, gain, table, wq, wk, wv, wo)
        return pl.pallas_call(
            _last,
            out_shape=jax.ShapeDtypeStruct((own, d), bf16),
            in_specs=[vmem] * 3,
            out_specs=anywhere,
            scratch_shapes=[pltpu.VMEM((own, d), bf16), dma((d // tile,))],
            compiler_params=pltpu.CompilerParams(vmem_limit_bytes=LAST_LIMIT),
        )(o, y, w)

    tokens, whole = P(("dp", "sp"), None), P(None, None)
    return jax.shard_map(
        step,
        mesh=mesh,
        in_specs=(tokens, P(None), whole, whole, whole, whole),
        out_specs=tokens,
        check_vma=False,
    )
```

```python
import functools

import jax
import jax.numpy as jnp
import numpy as np
from jax import lax
from jax.experimental import pallas as pl
from jax.experimental.pallas import tpu as pltpu
from jax.sharding import PartitionSpec as P

HEAD = 256
THETA = 10000
LOG2E = 1.4426950408889634
NEG = -1e30
VMEM_LIMIT = 52 * 2**20
LAST_LIMIT = 8 * 2**20
MESH = pl.DeviceIdType.MESH


def _dot(a, b, ca=1, cb=0):
    return lax.dot_general(a, b, (((ca,), (cb,)), ((), ())), preferred_element_type=jnp.float32)


def _kernel(x_hbm, gain_hbm, turn_hbm, wq_hbm, wk_hbm, wv_hbm, wo_hbm, o_s, y_s, wo_last,
            x_s, gain_s, turn_s, wk_s, wv_s, wq_s, wo_s, a_s, q_s, kv_s, acc_s, m_s, l_s, p_s,
            in_sem, wk_sem, wv_sem, wq_sem, wo_sem, send_sem, recv_sem, *, n):
    own, d = x_s.shape
    kv_heads, per = q_s.shape[0], q_s.shape[1] // own
    heads = kv_heads * per
    hh = HEAD // 2
    rounds, wide_q = wq_s.shape[0], wq_s.shape[2]
    group = wide_q // HEAD
    tile = 512
    tiles = d // tile
    me = lax.axis_index("sp")
    right, left = lax.rem(me + 1, n), lax.rem(me + n - 1, n)
    K, V = 0, 1
    R, L = 0, 1

    barrier = pltpu.get_barrier_semaphore()
    for peer in (left, right):
        pl.semaphore_signal(barrier, inc=1, device_id={"sp": peer}, device_id_type=MESH)

    def cols(i, width):
        return pl.ds(i * width if isinstance(i, int) else pl.multiple_of(i * width, width), width)

    x_in = pltpu.make_async_copy(x_hbm, x_s, in_sem.at[0])
    gain_in = pltpu.make_async_copy(gain_hbm, gain_s, in_sem.at[1])
    turn_in = pltpu.make_async_copy(turn_hbm.at[pl.ds(me * own, own)], turn_s, in_sem.at[2])

    def wk_in(h):
        return pltpu.make_async_copy(wk_hbm.at[:, cols(h, HEAD)], wk_s.at[h], wk_sem.at[h])

    def wv_in(h):
        return pltpu.make_async_copy(wv_hbm.at[:, cols(h, HEAD)], wv_s.at[h], wv_sem.at[h])

    def wq_in(i):
        return pltpu.make_async_copy(wq_hbm.at[:, cols(i, wide_q)], wq_s.at[i], wq_sem.at[i])

    def wo_in(h):
        return pltpu.make_async_copy(wo_hbm.at[cols(h, per * HEAD)], wo_last if h else wo_s, wo_sem.at[h])

    x_in.start()
    gain_in.start()
    wk_in(0).start()
    turn_in.start()
    gain_in.wait()
    for h in range(kv_heads):
        if h > 0:
            wk_in(h).start()
        wv_in(h).start()

    x_in.wait()
    for i in range(rounds):
        wq_in(i).start()
    wide = x_s[...].astype(jnp.float32)
    scale = lax.rsqrt(jnp.mean(wide * wide, -1, keepdims=True) + 1e-6)
    a_s[...] = (wide * scale * gain_s[...].astype(jnp.float32).reshape(1, d)).astype(jnp.bfloat16)

    def turn(t):
        t = t.astype(jnp.bfloat16).astype(jnp.float32)
        a, b = t[:, :hh], t[:, hh:]
        cos, sin = turn_s[:, :hh], turn_s[:, hh:]
        return (a * cos - b * sin).astype(jnp.bfloat16), (b * cos + a * sin).astype(jnp.bfloat16)

    def push(block, h, c, way):
        place = (block * kv_heads + h) * 2 + c
        pair = kv_heads * 2
        out = block % 2 * pair + h * 2 + c if way == R else pair + h * 2 + c if block == 0 else 2 * pair + h
        return pltpu.make_async_remote_copy(
            src_ref=kv_s.at[block, h, c], dst_ref=kv_s.at[block, h, c], send_sem=send_sem.at[out],
            recv_sem=recv_sem.at[place], device_id={"sp": left if way else right}, device_id_type=MESH)

    def arrived(block, h, c):
        push(block, h, c, R).wait_recv()

    def start_own(h, c):
        @pl.when(me == 0)
        def _():
            push(0, h, c, R).start()
            if h == 0:
                push(0, h, c, L).start()

        @pl.when(me == 1)
        def _():
            push(1, h, c, R).start()
            if c == V:
                push(1, h, c, L).start()

        if h == 0:
            @pl.when(me == 2)
            def _():
                push(2, h, c, R).start()

    def start_later():
        @pl.when(me == 0)
        def _():
            arrived(1, 0, V)
            push(1, 0, V, L).start()
            push(0, 1, K, L).start()
            push(0, 1, V, L).start()

        @pl.when(me == 2)
        def _():
            arrived(1, 0, K)
            push(1, 0, K, R).start()
            push(2, 1, K, R).start()

        @pl.when(me == 3)
        def _():
            arrived(0, 0, K)
            push(0, 0, K, L).start()

    def wait_sent():
        @pl.when(me == 0)
        def _():
            for h in range(kv_heads):
                for c in (K, V):
                    push(0, h, c, R).wait_send()
                    push(0, h, c, L).wait_send()
                push(1, h, V, L).wait_send()

        @pl.when(me == 1)
        def _():
            for h in range(kv_heads):
                for c in (K, V):
                    push(1, h, c, R).wait_send()
                push(1, h, V, L).wait_send()
            for c in (K, V):
                push(0, 1, c, R).wait_send()

        @pl.when(me == 2)
        def _():
            for h in range(kv_heads):
                for c in (K, V):
                    push(2, h, c, R).wait_send()
                push(1, h, K, R).wait_send()

        @pl.when(me == 3)
        def _():
            for c in (K, V):
                push(0, 0, c, L).wait_send()

    for h in range(kv_heads):
        wk_in(h).wait()
        if h == 0:
            turn_in.wait()
        k1, k2 = turn(_dot(a_s[...], wk_s[h]))
        kv_s[me, h, K, :, :hh] = k1
        kv_s[me, h, K, :, hh:] = k2
        if h == 0:
            pl.semaphore_wait(barrier, 2)
        start_own(h, K)
        wv_in(h).wait()
        kv_s[me, h, V] = _dot(a_s[...], wv_s[h]).astype(jnp.bfloat16)
        start_own(h, V)


    def query(i, _):
        wq_in(i).wait()
        for h in range(kv_heads):
            @pl.when(i == 1 + h)
            def _():
                wo_in(h).start()

        for r in range(group):
            j = i * group + r
            q1, q2 = turn(_dot(a_s[...], wq_s[i, :, r * HEAD:(r + 1) * HEAD]))
            rows = pl.ds(pl.multiple_of(lax.rem(j, per) * own, own), own)
            q_s[lax.div(j, per), rows, :hh] = q1
            q_s[lax.div(j, per), rows, hh:] = q2

        @pl.when(i == 1)
        def _():
            start_later()

    lax.fori_loop(0, rounds, query, None)
    y_s[...] = x_s[...].astype(jnp.float32)

    e = HEAD**-0.5 * LOG2E
    strips = [slice(r * own, (r + 1) * own) for r in range(per)]

    def scores(h, at, blocks, diagonal):
        out = [_dot(q_s[h, at], kv_s[b, h, K], 1, 1) for b in blocks]
        if diagonal:
            seen = lax.broadcasted_iota(jnp.int32, (own, own), 0) >= lax.broadcasted_iota(jnp.int32, (own, own), 1)
            out[0] = jnp.where(seen, out[0], NEG)
        return out

    def largest(parts, old=None):
        top = None
        for s in parts:
            for j in range(0, own, 128):
                top = s[:, j:j + 128] if top is None else jnp.maximum(top, s[:, j:j + 128])
        top = jnp.broadcast_to(jnp.max(top, axis=1, keepdims=True), (own, 128))
        return top if old is None else jnp.maximum(old, top)

    def weigh(parts, top):
        out, total = [], None
        for s in parts:
            for j in range(0, own, 128):
                p = jnp.exp2((s[:, j:j + 128] - top) * e)
                total = p if total is None else total + p
                out.append(p.astype(jnp.bfloat16))
        return jnp.concatenate(out, axis=1), total

    def twice(t):
        return jnp.concatenate([t, t], axis=1)

    def values(h, blocks):
        return jnp.concatenate([kv_s[b, h, V] for b in blocks], axis=0)

    def begin(h, blocks):
        def finish(p, at):
            acc_s[h, at] = _dot(p, values(h, blocks))

        later, prev = scores(h, strips[0], blocks, True), None
        for r, at in enumerate(strips):
            parts = later
            if r + 1 < per:
                later = scores(h, strips[r + 1], blocks, True)
            if prev is not None:
                finish(*prev)
            top = largest(parts)
            p, total = weigh(parts, top)
            m_s[h, at] = top
            l_s[h, at] = total
            prev = p, at
        finish(*prev)

    def project():
        for t in range(tiles):
            here = slice(t * tile, (t + 1) * tile)
            y_s[:, here] = y_s[:, here] + _dot(o_s[...], wo_s[:, here])

    def result(p, keep, total, h, blocks, r, at):
        share = 1 / jnp.broadcast_to(jnp.sum(total, axis=1, keepdims=True), (own, 128))
        mix = acc_s[h, at] * twice(keep) + _dot(p, values(h, blocks))
        o_s[:, r * HEAD:(r + 1) * HEAD] = (mix * twice(share)).astype(jnp.bfloat16)

    def rest(h, blocks, use):
        later = scores(h, strips[0], blocks, False)
        for r, at in enumerate(strips):
            parts = later
            if r + 1 < per:
                later = scores(h, strips[r + 1], blocks, False)
            old = m_s[h, at]
            top = largest(parts, old)
            p, total = weigh(parts, top)
            keep = jnp.exp2((old - top) * e)
            use(p, keep, l_s[h, at] * keep + total, r, at)
        use(None, None, None, per, None)

    def end(h, blocks):
        held = []

        def use(p, keep, total, r, at):
            if held:
                result(*held.pop())
            held.append((p, keep, total, h, blocks, r, at))

        rest(h, blocks, use)

    def weigh_rest(h, blocks):
        def use(p, keep, total, r, at):
            if r < per:
                p_s[at, :len(blocks) * own] = p
                m_s[h, at] = keep
                l_s[h, at] = total

        rest(h, blocks, use)

    def end_rest(h, blocks):
        for r, at in enumerate(strips):
            result(p_s[at, :len(blocks) * own], m_s[h, at], l_s[h, at], h, blocks, r, at)

    def end_alone(h):
        for r, at in enumerate(strips):
            share = 1 / jnp.broadcast_to(jnp.sum(l_s[h, at], axis=1, keepdims=True), (own, 128))
            o_s[:, r * HEAD:(r + 1) * HEAD] = (acc_s[h, at] * twice(share)).astype(jnp.bfloat16)


    @pl.when(me == 0)
    def _():
        arrived(1, 1, V)
        push(1, 1, V, L).start()

    def head(h, _):
        first, second = h == 0, h > 0

        @pl.when((me == 3) & first)
        def _():
            arrived(0, 0, V)
            push(0, 0, V, L).start()
            arrived(2, 0, K)

        @pl.when((me >= 2) & first)
        def _():
            arrived(me - 1, 0, V)
            begin(0, [me, me - 1])

        @pl.when((me <= 1) | first)
        def _():
            begin(jnp.where(me <= 1, h, 1), [me])

        @pl.when(me == 0)
        def _():
            end_alone(h)

        @pl.when((me == 1) & first)
        def _():
            for c in (K, V):
                arrived(0, 0, c)
            arrived(0, 1, K)
            push(0, 1, K, R).start()

        @pl.when((me == 2) & first)
        def _():
            arrived(1, 1, K)
            push(1, 1, K, R).start()
            push(2, 1, V, R).start()
            for c in (K, V):
                arrived(0, 0, c)

        @pl.when((me == 1) | ((me == 2) & first))
        def _():
            end(h, [0])

        @pl.when((me == 1) & first)
        def _():
            arrived(0, 1, V)
            push(0, 1, V, R).start()

        @pl.when((me == 3) & first)
        def _():
            for c in (K, V):
                arrived(1, 0, c)
            end(h, [0, 1])

        @pl.when((me == 2) & second)
        def _():
            arrived(0, 1, K)
            weigh_rest(1, [1, 0])
            arrived(1, 1, V)
            arrived(0, 1, V)
            end_rest(1, [1, 0])

        @pl.when((me == 3) & second)
        def _():
            others = [0, 2, 1]
            for b in others:
                arrived(b, 1, K)
            weigh_rest(1, others)
            for b in others:
                arrived(b, 1, V)
            end_rest(1, others)

        @pl.when(first)
        def _():
            wo_in(0).wait()
            project()

    lax.fori_loop(0, kv_heads, head, None)
    wo_in(1).wait()
    wait_sent()


def _last(o_ref, y_ref, w_ref, out_hbm, out_s, sem):
    tiles = sem.shape[0]
    tile = out_s.shape[1] // tiles

    def leave(i):
        here = slice(i * tile, (i + 1) * tile)
        return pltpu.make_async_copy(out_s.at[:, here], out_hbm.at[:, here], sem.at[i])

    for i in range(tiles):
        here = slice(i * tile, (i + 1) * tile)
        out_s[:, here] = (y_ref[:, here] + _dot(o_ref[...], w_ref[:, here])).astype(out_s.dtype)
        leave(i).start()
    for i in range(tiles):
        leave(i).wait()


def solution(mesh):
    n = mesh.shape["sp"]

    def step(x, gain, wq, wk, wv, wo):
        own, d = x.shape
        heads, kv_heads = wq.shape[1] // HEAD, wk.shape[1] // HEAD
        per = heads // kv_heads
        tile, wide_q = 512, 1024
        place = np.arange(n * own, dtype=np.float64)[:, None]
        angle = place * THETA ** (-np.arange(HEAD // 2, dtype=np.float64) / (HEAD // 2))
        table = jnp.asarray(np.concatenate([np.cos(angle), np.sin(angle)], 1), jnp.float32)
        anywhere = pl.BlockSpec(memory_space=pl.ANY)
        dma = pltpu.SemaphoreType.DMA
        bf16, f32 = jnp.bfloat16, jnp.float32
        vmem = pl.BlockSpec(memory_space=pltpu.VMEM)
        o, y, w = pl.pallas_call(
            functools.partial(_kernel, n=n),
            out_shape=[pltpu.VMEM((own, per * HEAD), bf16), pltpu.VMEM((own, d), f32), pltpu.VMEM((per * HEAD, d), bf16)],
            in_specs=[anywhere] * 7,
            out_specs=[vmem] * 3,
            scratch_shapes=[
                pltpu.VMEM((own, d), bf16),
                pltpu.VMEM((d,), bf16),
                pltpu.VMEM((own, HEAD), f32),
                pltpu.VMEM((kv_heads, d, HEAD), bf16),
                pltpu.VMEM((kv_heads, d, HEAD), bf16),
                pltpu.VMEM((heads * HEAD // wide_q, d, wide_q), bf16),
                pltpu.VMEM((per * HEAD, d), bf16),
                pltpu.VMEM((own, d), bf16),
                pltpu.VMEM((kv_heads, per * own, HEAD), bf16),
                pltpu.VMEM((n, kv_heads, 2, own, HEAD), bf16),
                pltpu.VMEM((kv_heads, per * own, HEAD), f32),
                pltpu.VMEM((kv_heads, per * own, 128), f32),
                pltpu.VMEM((kv_heads, per * own, 128), f32),
                pltpu.VMEM((per * own, (n - 1) * own), bf16),
                dma((3,)), dma((kv_heads,)), dma((kv_heads,)), dma((heads * HEAD // wide_q,)), dma((kv_heads,)),
                dma((kv_heads * 5,)), dma(((n - 1) * kv_heads * 2,)),
            ],
            compiler_params=pltpu.CompilerParams(collective_id=0, has_side_effects=True, vmem_limit_bytes=VMEM_LIMIT),
        )(x, gain, table, wq, wk, wv, wo)
        return pl.pallas_call(
            _last,
            out_shape=jax.ShapeDtypeStruct((own, d), bf16),
            in_specs=[vmem] * 3,
            out_specs=anywhere,
            scratch_shapes=[pltpu.VMEM((own, d), bf16), dma((d // tile,))],
            compiler_params=pltpu.CompilerParams(vmem_limit_bytes=LAST_LIMIT),
        )(o, y, w)

    tokens, whole = P(("dp", "sp"), None), P(None, None)
    return jax.shard_map(
        step,
        mesh=mesh,
        in_specs=(tokens, P(None), whole, whole, whole, whole),
        out_specs=tokens,
        check_vma=False,
    )
```

```python
import functools

import jax
import jax.numpy as jnp
import numpy as np
from jax import lax
from jax.experimental import pallas as pl
from jax.experimental.pallas import tpu as pltpu
from jax.sharding import PartitionSpec as P

HEAD = 256
THETA = 10000
LOG2E = 1.4426950408889634
NEG = -1e30
VMEM_LIMIT = 52 * 2**20
LAST_LIMIT = 8 * 2**20
MESH = pl.DeviceIdType.MESH


def _dot(a, b, ca=1, cb=0):
    return lax.dot_general(a, b, (((ca,), (cb,)), ((), ())), preferred_element_type=jnp.float32)


def _kernel(x_hbm, gain_hbm, turn_hbm, wq_hbm, wk_hbm, wv_hbm, wo_hbm, o_s, y_s, wo_last,
            x_s, gain_s, turn_s, wk_s, wv_s, wq_s, wo_s, a_s, q_s, kv_s, acc_s, m_s, l_s, p_s,
            in_sem, wk_sem, wq_sem, wo_sem, send_sem, recv_sem, *, n):
    own, d = x_s.shape
    kv_heads, per = q_s.shape[0], q_s.shape[1] // own
    heads = kv_heads * per
    hh = HEAD // 2
    rounds, wide_q = wq_s.shape[0], wq_s.shape[2]
    group = wide_q // HEAD
    tile = 512
    tiles = d // tile
    me = lax.axis_index("sp")
    right, left = lax.rem(me + 1, n), lax.rem(me + n - 1, n)
    K, V = 0, 1
    R, L = 0, 1

    barrier = pltpu.get_barrier_semaphore()
    for peer in (left, right):
        pl.semaphore_signal(barrier, inc=1, device_id={"sp": peer}, device_id_type=MESH)

    def cols(i, width):
        return pl.ds(i * width if isinstance(i, int) else pl.multiple_of(i * width, width), width)

    x_in = pltpu.make_async_copy(x_hbm, x_s, in_sem.at[0])
    gain_in = pltpu.make_async_copy(gain_hbm, gain_s, in_sem.at[1])
    turn_in = pltpu.make_async_copy(turn_hbm.at[pl.ds(me * own, own)], turn_s, in_sem.at[2])

    def wk_in(h):
        return pltpu.make_async_copy(wk_hbm.at[:, cols(h, HEAD)], wk_s.at[h], wk_sem.at[h])

    wv_in = pltpu.make_async_copy(wv_hbm, wv_s, in_sem.at[3])

    def wq_in(i):
        return pltpu.make_async_copy(wq_hbm.at[:, cols(i, wide_q)], wq_s.at[i], wq_sem.at[i])

    def wo_in(h):
        return pltpu.make_async_copy(wo_hbm.at[cols(h, per * HEAD)], wo_last if h else wo_s, wo_sem.at[h])

    x_in.start()
    gain_in.start()
    wk_in(0).start()
    turn_in.start()
    gain_in.wait()
    wv_in.start()
    for h in range(1, kv_heads):
        wk_in(h).start()

    x_in.wait()
    for i in range(rounds):
        wq_in(i).start()
    wide = x_s[...].astype(jnp.float32)
    scale = lax.rsqrt(jnp.mean(wide * wide, -1, keepdims=True) + 1e-6)
    a_s[...] = (wide * scale * gain_s[...].astype(jnp.float32).reshape(1, d)).astype(jnp.bfloat16)

    def turn(t):
        t = t.astype(jnp.bfloat16).astype(jnp.float32)
        a, b = t[:, :hh], t[:, hh:]
        cos, sin = turn_s[:, :hh], turn_s[:, hh:]
        return (a * cos - b * sin).astype(jnp.bfloat16), (b * cos + a * sin).astype(jnp.bfloat16)

    def push(block, h, c, way):
        place = (block * kv_heads + h) * 2 + c
        pair = kv_heads * 2
        out = block % 2 * pair + h * 2 + c if way == R else pair + h * 2 + c if block == 0 else 2 * pair + h
        return pltpu.make_async_remote_copy(
            src_ref=kv_s.at[block, h, c], dst_ref=kv_s.at[block, h, c], send_sem=send_sem.at[out],
            recv_sem=recv_sem.at[place], device_id={"sp": left if way else right}, device_id_type=MESH)

    def arrived(block, h, c):
        push(block, h, c, R).wait_recv()

    def start_own(h, c):
        @pl.when(me == 0)
        def _():
            push(0, h, c, R).start()
            if h == 0:
                push(0, h, c, L).start()

        @pl.when(me == 1)
        def _():
            push(1, h, c, R).start()
            if c == V:
                push(1, h, c, L).start()

        if h == 0:
            @pl.when(me == 2)
            def _():
                push(2, h, c, R).start()

    def start_later():
        @pl.when(me == 0)
        def _():
            arrived(1, 0, V)
            push(1, 0, V, L).start()
            push(0, 1, K, L).start()
            push(0, 1, V, L).start()

        @pl.when(me == 2)
        def _():
            arrived(1, 0, K)
            push(1, 0, K, R).start()
            push(2, 1, K, R).start()

        @pl.when(me == 3)
        def _():
            arrived(0, 0, K)
            push(0, 0, K, L).start()

    def wait_sent():
        @pl.when(me == 0)
        def _():
            for h in range(kv_heads):
                for c in (K, V):
                    push(0, h, c, R).wait_send()
                    push(0, h, c, L).wait_send()
                push(1, h, V, L).wait_send()

        @pl.when(me == 1)
        def _():
            for h in range(kv_heads):
                for c in (K, V):
                    push(1, h, c, R).wait_send()
                push(1, h, V, L).wait_send()
            for c in (K, V):
                push(0, 1, c, R).wait_send()

        @pl.when(me == 2)
        def _():
            for h in range(kv_heads):
                for c in (K, V):
                    push(2, h, c, R).wait_send()
                push(1, h, K, R).wait_send()

        @pl.when(me == 3)
        def _():
            for c in (K, V):
                push(0, 0, c, L).wait_send()

    for h in range(kv_heads):
        wk_in(h).wait()
        if h == 0:
            turn_in.wait()
        k1, k2 = turn(_dot(a_s[...], wk_s[h]))
        kv_s[me, h, K, :, :hh] = k1
        kv_s[me, h, K, :, hh:] = k2
        if h == 0:
            pl.semaphore_wait(barrier, 2)
        start_own(h, K)
        if h == 0:
            wv_in.wait()
        kv_s[me, h, V] = _dot(a_s[...], wv_s[:, h * HEAD:(h + 1) * HEAD]).astype(jnp.bfloat16)
        start_own(h, V)


    def query(i, _):
        wq_in(i).wait()
        for h in range(kv_heads):
            @pl.when(i == 1 + h)
            def _():
                wo_in(h).start()

        for r in range(group):
            j = i * group + r
            q1, q2 = turn(_dot(a_s[...], wq_s[i, :, r * HEAD:(r + 1) * HEAD]))
            rows = pl.ds(pl.multiple_of(lax.rem(j, per) * own, own), own)
            q_s[lax.div(j, per), rows, :hh] = q1
            q_s[lax.div(j, per), rows, hh:] = q2

        @pl.when(i == 1)
        def _():
            start_later()

    lax.fori_loop(0, rounds, query, None)
    y_s[...] = x_s[...].astype(jnp.float32)

    e = HEAD**-0.5 * LOG2E
    strips = [slice(r * own, (r + 1) * own) for r in range(per)]

    def scores(h, at, blocks, diagonal):
        out = [_dot(q_s[h, at], kv_s[b, h, K], 1, 1) for b in blocks]
        if diagonal:
            seen = lax.broadcasted_iota(jnp.int32, (own, own), 0) >= lax.broadcasted_iota(jnp.int32, (own, own), 1)
            out[0] = jnp.where(seen, out[0], NEG)
        return out

    def largest(parts, old=None):
        top = None
        for s in parts:
            for j in range(0, own, 128):
                top = s[:, j:j + 128] if top is None else jnp.maximum(top, s[:, j:j + 128])
        top = jnp.broadcast_to(jnp.max(top, axis=1, keepdims=True), (own, 128))
        return top if old is None else jnp.maximum(old, top)

    def weigh(parts, top):
        out, total = [], None
        for s in parts:
            for j in range(0, own, 128):
                p = jnp.exp2((s[:, j:j + 128] - top) * e)
                total = p if total is None else total + p
                out.append(p.astype(jnp.bfloat16))
        return jnp.concatenate(out, axis=1), total

    def twice(t):
        return jnp.concatenate([t, t], axis=1)

    def values(h, blocks):
        return jnp.concatenate([kv_s[b, h, V] for b in blocks], axis=0)

    def begin(h, blocks):
        def finish(p, at):
            acc_s[h, at] = _dot(p, values(h, blocks))

        later, prev = scores(h, strips[0], blocks, True), None
        for r, at in enumerate(strips):
            parts = later
            if r + 1 < per:
                later = scores(h, strips[r + 1], blocks, True)
            if prev is not None:
                finish(*prev)
            top = largest(parts)
            p, total = weigh(parts, top)
            m_s[h, at] = top
            l_s[h, at] = total
            prev = p, at
        finish(*prev)

    def project():
        for t in range(tiles):
            here = slice(t * tile, (t + 1) * tile)
            y_s[:, here] = y_s[:, here] + _dot(o_s[...], wo_s[:, here])

    def result(p, keep, total, h, blocks, r, at):
        share = 1 / jnp.broadcast_to(jnp.sum(total, axis=1, keepdims=True), (own, 128))
        mix = acc_s[h, at] * twice(keep) + _dot(p, values(h, blocks))
        o_s[:, r * HEAD:(r + 1) * HEAD] = (mix * twice(share)).astype(jnp.bfloat16)

    def rest(h, blocks, use):
        later = scores(h, strips[0], blocks, False)
        for r, at in enumerate(strips):
            parts = later
            if r + 1 < per:
                later = scores(h, strips[r + 1], blocks, False)
            old = m_s[h, at]
            top = largest(parts, old)
            p, total = weigh(parts, top)
            keep = jnp.exp2((old - top) * e)
            use(p, keep, l_s[h, at] * keep + total, r, at)
        use(None, None, None, per, None)

    def end(h, blocks):
        held = []

        def use(p, keep, total, r, at):
            if held:
                result(*held.pop())
            held.append((p, keep, total, h, blocks, r, at))

        rest(h, blocks, use)

    def weigh_rest(h, blocks):
        def use(p, keep, total, r, at):
            if r < per:
                p_s[at, :len(blocks) * own] = p
                m_s[h, at] = keep
                l_s[h, at] = total

        rest(h, blocks, use)

    def end_rest(h, blocks):
        for r, at in enumerate(strips):
            result(p_s[at, :len(blocks) * own], m_s[h, at], l_s[h, at], h, blocks, r, at)

    def end_alone(h):
        for r, at in enumerate(strips):
            share = 1 / jnp.broadcast_to(jnp.sum(l_s[h, at], axis=1, keepdims=True), (own, 128))
            o_s[:, r * HEAD:(r + 1) * HEAD] = (acc_s[h, at] * twice(share)).astype(jnp.bfloat16)


    @pl.when(me == 0)
    def _():
        arrived(1, 1, V)
        push(1, 1, V, L).start()

    def head(h, _):
        first, second = h == 0, h > 0

        @pl.when((me == 3) & first)
        def _():
            arrived(0, 0, V)
            push(0, 0, V, L).start()
            arrived(2, 0, K)

        @pl.when((me >= 2) & first)
        def _():
            arrived(me - 1, 0, V)
            begin(0, [me, me - 1])

        @pl.when((me <= 1) | first)
        def _():
            begin(jnp.where(me <= 1, h, 1), [me])

        @pl.when(me == 0)
        def _():
            end_alone(h)

        @pl.when((me == 1) & first)
        def _():
            for c in (K, V):
                arrived(0, 0, c)
            arrived(0, 1, K)
            push(0, 1, K, R).start()

        @pl.when((me == 2) & first)
        def _():
            arrived(1, 1, K)
            push(1, 1, K, R).start()
            push(2, 1, V, R).start()
            for c in (K, V):
                arrived(0, 0, c)

        @pl.when((me == 1) | ((me == 2) & first))
        def _():
            end(h, [0])

        @pl.when((me == 1) & first)
        def _():
            arrived(0, 1, V)
            push(0, 1, V, R).start()

        @pl.when((me == 3) & first)
        def _():
            for c in (K, V):
                arrived(1, 0, c)
            end(h, [0, 1])

        @pl.when((me == 2) & second)
        def _():
            arrived(0, 1, K)
            weigh_rest(1, [1, 0])
            arrived(1, 1, V)
            arrived(0, 1, V)
            end_rest(1, [1, 0])

        @pl.when((me == 3) & second)
        def _():
            others = [0, 2, 1]
            for b in others:
                arrived(b, 1, K)
            weigh_rest(1, others)
            for b in others:
                arrived(b, 1, V)
            end_rest(1, others)

        @pl.when(first)
        def _():
            wo_in(0).wait()
            project()

    lax.fori_loop(0, kv_heads, head, None)
    wo_in(1).wait()
    wait_sent()


def _last(o_ref, y_ref, w_ref, out_hbm, out_s, sem):
    tiles = sem.shape[0]
    tile = out_s.shape[1] // tiles

    def leave(i):
        here = slice(i * tile, (i + 1) * tile)
        return pltpu.make_async_copy(out_s.at[:, here], out_hbm.at[:, here], sem.at[i])

    for i in range(tiles):
        here = slice(i * tile, (i + 1) * tile)
        out_s[:, here] = (y_ref[:, here] + _dot(o_ref[...], w_ref[:, here])).astype(out_s.dtype)
        leave(i).start()
    for i in range(tiles):
        leave(i).wait()


def solution(mesh):
    n = mesh.shape["sp"]

    def step(x, gain, wq, wk, wv, wo):
        own, d = x.shape
        heads, kv_heads = wq.shape[1] // HEAD, wk.shape[1] // HEAD
        per = heads // kv_heads
        tile, wide_q = 512, 1024
        place = np.arange(n * own, dtype=np.float64)[:, None]
        angle = place * THETA ** (-np.arange(HEAD // 2, dtype=np.float64) / (HEAD // 2))
        table = jnp.asarray(np.concatenate([np.cos(angle), np.sin(angle)], 1), jnp.float32)
        anywhere = pl.BlockSpec(memory_space=pl.ANY)
        dma = pltpu.SemaphoreType.DMA
        bf16, f32 = jnp.bfloat16, jnp.float32
        vmem = pl.BlockSpec(memory_space=pltpu.VMEM)
        o, y, w = pl.pallas_call(
            functools.partial(_kernel, n=n),
            out_shape=[pltpu.VMEM((own, per * HEAD), bf16), pltpu.VMEM((own, d), f32), pltpu.VMEM((per * HEAD, d), bf16)],
            in_specs=[anywhere] * 7,
            out_specs=[vmem] * 3,
            scratch_shapes=[
                pltpu.VMEM((own, d), bf16),
                pltpu.VMEM((d,), bf16),
                pltpu.VMEM((own, HEAD), f32),
                pltpu.VMEM((kv_heads, d, HEAD), bf16),
                pltpu.VMEM((d, kv_heads * HEAD), bf16),
                pltpu.VMEM((heads * HEAD // wide_q, d, wide_q), bf16),
                pltpu.VMEM((per * HEAD, d), bf16),
                pltpu.VMEM((own, d), bf16),
                pltpu.VMEM((kv_heads, per * own, HEAD), bf16),
                pltpu.VMEM((n, kv_heads, 2, own, HEAD), bf16),
                pltpu.VMEM((kv_heads, per * own, HEAD), f32),
                pltpu.VMEM((kv_heads, per * own, 128), f32),
                pltpu.VMEM((kv_heads, per * own, 128), f32),
                pltpu.VMEM((per * own, (n - 1) * own), bf16),
                dma((4,)), dma((kv_heads,)), dma((heads * HEAD // wide_q,)), dma((kv_heads,)),
                dma((kv_heads * 5,)), dma(((n - 1) * kv_heads * 2,)),
            ],
            compiler_params=pltpu.CompilerParams(collective_id=0, has_side_effects=True, vmem_limit_bytes=VMEM_LIMIT),
        )(x, gain, table, wq, wk, wv, wo)
        return pl.pallas_call(
            _last,
            out_shape=jax.ShapeDtypeStruct((own, d), bf16),
            in_specs=[vmem] * 3,
            out_specs=anywhere,
            scratch_shapes=[pltpu.VMEM((own, d), bf16), dma((d // tile,))],
            compiler_params=pltpu.CompilerParams(vmem_limit_bytes=LAST_LIMIT),
        )(o, y, w)

    tokens, whole = P(("dp", "sp"), None), P(None, None)
    return jax.shard_map(
        step,
        mesh=mesh,
        in_specs=(tokens, P(None), whole, whole, whole, whole),
        out_specs=tokens,
        check_vma=False,
    )
```
